768 devices in a mesh: gx: 64 (over y, x, core), gy: 12 (over z).
Axes of the slice: x: 4, y: 8, z: 12, core: 2. Of those that a mesh axis runs over, the one named last changes fastest.
Arguments:
- displacement: float32 [3, 128, 24, 128], P(None, 'gx', 'gy'), may hold values from -0.3 to 0.3
- velocity: float32 [3, 128, 24, 128], P(None, 'gx', 'gy'), may hold values from -30 to 30
- forces: float32 [3, 128, 24, 128], P(None, 'gx', 'gy'), may hold values from -30 to 30
- heights: int32 [128, 24, 128], P('gx', 'gy'), may hold values from 0 to 127, as said below
- counts: int32 [128, 24], P('gx', 'gy'), may hold values from 64 to 128
- neighbours: int32 [8, 128, 24, 128], P(None, 'gx', 'gy'), may hold values from 0 to 1151, as said below
- plan: int32 [64, 12, 4, 1], P('gx', 'gy'), may hold values from 0 to 11; in each aligned block of 4 rows (0 to 3, 4 to 7, ..., all dimensions but the last counted through in order) at most 2 rows name the same one
Outputs:
- arrived: float32 [64, 12, 12, 2, 7, 128], P('gx', 'gy')
The draws below stay inside these ranges and needn't reach their ends.
Inputs may be any that keep to these rules, and one draw needn't show every extreme that they name: `heights`: each cell column's 128 entries name every layer from 0 to 127 once. `neighbours`: entry c * 128 + s names slot s of the column at offset (c // 3 - 1, c % 3 - 1) in x and y; a slot never names itself. `plan`: among one device's 2 * 2 cell columns at most 2 name the same new owner.
All inputs are finite; a program needn't handle non-finite values.
Results may differ from the reference program's by a relative error of at most 0.0003.
Values sent between devices are 32-bit elements; how exact they have to be, the bound alone decides.
A program may use at most 32 MiB of HBM per device.

```python
import math
import jax
import jax.numpy as jnp
import numpy as np
from jax import lax

CX = 2
CY = 2
S = 128
K = 8
STEPS = 1
NXC = 128
NYC = 24
CAP = 2
N_GX = 64
N_GY = 12


def layout_tables(key):
    base_key = jax.random.fold_in(key, 11)
    key_order, key_cell, key_slot, key_shuffle = jax.random.split(base_key, 4)
    ramp = jnp.arange(S, dtype=jnp.int32)
    scores = jax.random.randint(key_order, (NXC, NYC, S), 0, 1 << 20) * S + ramp
    layers = jnp.argsort(scores, axis=-1).astype(jnp.int32)
    slot_of = jnp.argsort(layers, axis=-1).astype(jnp.int32)
    entries = []
    for shift_x, shift_y in ((-1, 0), (1, 0), (0, -1), (0, 1)):
        position = (shift_x + 1) * 3 + (shift_y + 1)
        moved = jnp.roll(jnp.roll(slot_of, -shift_x, axis=0), -shift_y, axis=1)
        entries.append(position * S + jnp.take_along_axis(moved, layers, axis=2))
    for change in (-1, 1):
        target = (layers + change + S) % S
        entries.append(4 * S + jnp.take_along_axis(slot_of, target, axis=2))
    extra_cell = jax.random.randint(key_cell, (2, NXC, NYC, S), 0, 8)
    extra_cell = extra_cell + (extra_cell >= 4).astype(jnp.int32)
    extra_slot = jax.random.randint(key_slot, (2, NXC, NYC, S), 0, S)
    entries.append(extra_cell[0] * S + extra_slot[0])
    entries.append(extra_cell[1] * S + extra_slot[1])
    lists = jnp.stack(entries, axis=0).astype(jnp.int32)
    shuffle_scores = jax.random.randint(key_shuffle, (8, NXC, NYC, S), 0, 1 << 20) * 8 + jnp.arange(8, dtype=jnp.int32)[:, None, None, None]
    order = jnp.argsort(shuffle_scores, axis=0)
    lists = jnp.take_along_axis(lists, order, axis=0).astype(jnp.int32)
    return (layers, lists)


def draw_heights(key, part):
    layers, lists = layout_tables(key)
    return layers


def draw_neighbours(key, part):
    layers, lists = layout_tables(key)
    return lists


def place_ends(drawn, own_key, low, top_value):
    spot = [jax.random.randint(jax.random.fold_in(own_key, axis), (), 0, length) for axis, length in enumerate(drawn.shape)]
    widest = drawn.shape.index(max(drawn.shape))
    beside = spot[:widest] + [(spot[widest] + 1) % drawn.shape[widest]] + spot[widest + 1:]
    return drawn.at[tuple(spot)].set(low).at[tuple(beside)].set(top_value)


def shard_levels(own_key, dims, shards, least, high):
    gain, own = 1.0, jax.random.fold_in(own_key, 6)
    for axis_at, blocks in shards:
        steps = jnp.exp(jax.random.uniform(jax.random.fold_in(own, axis_at), (blocks,), jnp.float32, least / len(shards), high / len(shards)))
        gain = gain * jnp.repeat(steps, dims[axis_at] // blocks).reshape([-1 if axis == axis_at else 1 for axis in range(len(dims))])
    return gain


def deal_out(stream_key, own, number, rows, amount, top, reach, lean):
    sequence = jax.random.permutation(stream_key, amount)
    crowded, ordinary = load_shares(amount, rows * top, reach, lean, True), load_shares(amount, rows * top, reach, lean, False)
    places = jnp.arange(amount)

    def named(lengths, offset_by):
        used = int((lengths > 0).sum())
        fixed = max(1, used // 4)
        passed = fixed + (places - fixed + offset_by * (used - fixed)) % max(1, amount - fixed)
        return jnp.zeros((amount,), jnp.int32).at[sequence[jnp.where(places < fixed, places, passed)]].set(jnp.asarray(lengths, jnp.int32))

    lengths = jnp.where(number % 4 == 0, named(crowded, number // 4), named(ordinary, number - number // 4 - 1))
    mixed = jax.random.permutation(jax.random.fold_in(own, 3), amount)
    giver, taker = mixed[0:amount // 2 * 2:2], mixed[1:amount // 2 * 2:2]
    slack = jnp.minimum(lengths[giver] - 1, reach - lengths[taker]) // 2
    slack = jnp.where((giver == sequence[0]) | (taker == sequence[0]) | (lengths[taker] == 0), 0, jnp.maximum(slack, 0))
    passed = jax.random.randint(jax.random.fold_in(own, 4), (amount // 2,), 0, 1 << 20) % (slack + 1)
    lengths = lengths.at[giver].add(-passed).at[taker].add(passed)
    members = jnp.searchsorted(jnp.cumsum(lengths), jnp.arange(rows * top), side="right").astype(jnp.int32)
    grid = members.reshape(top, rows).T
    grid = grid[jax.random.permutation(jax.random.fold_in(own, 1), rows)]
    offset_by = jax.random.randint(jax.random.fold_in(own, 2), (rows, 1), 0, top)
    return jnp.take_along_axis(grid, (jnp.arange(top)[None, :] + offset_by) % top, axis=1)


def load_shares(count, total, limit, lean, full):
    loads = [(1 << 20) // math.isqrt(grade ** lean) + 1 for grade in range(1, count + 1)]
    largest = limit if full else min(limit, max(-(-total // count), total * loads[0] // sum(loads)))
    least = 1 if total - largest >= count - 1 else 0
    given, spare = [largest] + [least] * (count - 1), total - largest - least * (count - 1)
    while spare > 0:
        candidates = [i for i in range(1, count) if given[i] < largest] or [i for i in range(1, count) if given[i] < limit]
        pool, remaining = sum([loads[i] for i in candidates]), spare
        for i in candidates:
            extra = min(limit - given[i], max(1, remaining * loads[i] // pool), spare)
            given[i] = given[i] + extra
            spare = spare - extra
    return np.array(given)


def bell_draw(rng, dims, width, bound, cuts=(), kind=jnp.bfloat16):
    values = width * jax.random.normal(rng, dims, jnp.float32)
    if cuts:
        values = values * shard_levels(rng, dims, cuts, -0.22, 0.18)
    return jnp.clip(values, -bound, bound).astype(kind)


def setup_inputs(seed: int = 0) -> dict:
    keys = jax.random.split(jax.random.key(seed), 8)
    displacement = bell_draw(keys[0], (3, NXC, NYC, S), 0.1, 0.3, ((1, 64), (2, 12)), jnp.float32)
    velocity = bell_draw(keys[1], (3, NXC, NYC, S), 5.0, 30.0, ((1, 64), (2, 12)), jnp.float32)
    forces = bell_draw(keys[2], (3, NXC, NYC, S), 5.0, 30.0, ((1, 64), (2, 12)), jnp.float32)
    heights = draw_heights(jax.random.fold_in(keys[7], 71), 0)
    counts = place_ends(jax.random.randint(keys[4], (NXC, NYC), S // 2, S + 1), jax.random.fold_in(keys[4], 1), S // 2, S).astype(jnp.int32)
    neighbours = draw_neighbours(jax.random.fold_in(keys[7], 71), 0)
    plan_keys = jax.random.split(jax.random.fold_in(keys[6], 1), N_GX * N_GY * (CX * CY) // (CX * CY))
    plan_turns = jax.random.permutation(jax.random.fold_in(keys[6], 3), N_GX * N_GY * (CX * CY) // (CX * CY))
    plan = jax.vmap(lambda own, number: deal_out(jax.random.fold_in(keys[6], 2), own, number, CX * CY, N_GY, 1, CAP, 2))(plan_keys, plan_turns).reshape((N_GX, N_GY, CX * CY, 1))
    return dict(displacement=displacement, velocity=velocity, forces=forces, heights=heights, counts=counts, neighbours=neighbours, plan=plan)


repulse_a = 1830.8
attract_b = 471.18
decay_one = 2.4799
decay_two = 1.7322
beta_t = 1.1e-06
expo_n = 0.78734
coeff_c2 = 100390.0 ** 2
coeff_d2 = 16.217 ** 2
coeff_h = -0.59825
spacing = 2.4
time_step = 0.001
half_step = 0.0005
force_scale = 9648.53 / 28.0855

def cutoff(radius):
    smooth = 0.5 - 0.5 * jnp.sin(0.5 * jnp.pi * (radius - 2.85) / 0.15)
    return jnp.where(radius < 2.7, 1.0, jnp.where(radius > 3.0, 0.0, smooth))

def cell_energy(center, nearby):
    offsets = nearby[:3] - center[:3][:, :, :, None, :]
    radius = jnp.sqrt(jnp.maximum(lax.optimization_barrier(jnp.sum(offsets * offsets, axis=0)), 1.0))
    weight = cutoff(radius) * nearby[3]
    direction = offsets / radius
    cosine = direction[0][:, :, :, None, :] * direction[0][:, :, None, :, :]
    cosine = cosine + direction[1][:, :, :, None, :] * direction[1][:, :, None, :, :]
    cosine = cosine + direction[2][:, :, :, None, :] * direction[2][:, :, None, :, :]
    spread = (coeff_h - cosine) ** 2
    angular = 1.0 + coeff_c2 * spread / (coeff_d2 * (coeff_d2 + spread))
    others = 1.0 - jnp.eye(nearby.shape[3], dtype=cosine.dtype)[:, :, None]
    bond_sum = jnp.maximum(lax.optimization_barrier(jnp.sum(angular * weight[:, :, None, :, :] * others, axis=3)), 1.0)
    bond_order = (1.0 + jnp.exp(expo_n * jnp.log(beta_t * bond_sum))) ** (-0.5 / expo_n)
    pair_terms = weight * (repulse_a * jnp.exp(-decay_one * radius) - attract_b * jnp.exp(-decay_two * radius) * bond_order)
    return 0.5 * center[3] * lax.optimization_barrier(jnp.sum(pair_terms, axis=2))

def flat_index(neighbours):
    width_x, width_y = (neighbours.shape[1], neighbours.shape[2])
    return jnp.transpose(neighbours, (1, 2, 0, 3)).reshape(width_x, width_y, -1)

def gather_nearby(points, gather_index):
    width_x, width_y = (gather_index.shape[0], gather_index.shape[1])
    slots = points.shape[3]
    pieces = [points[:, 1 + shift_x:1 + shift_x + width_x, 1 + shift_y:1 + shift_y + width_y] for shift_x in (-1, 0, 1) for shift_y in (-1, 0, 1)]
    joined = jnp.concatenate(pieces, axis=3)
    wide_index = jnp.broadcast_to(gather_index[None], (4,) + gather_index.shape)
    picked = jnp.take_along_axis(joined, wide_index, axis=3)
    return picked.reshape(4, width_x, width_y, gather_index.shape[2] // slots, slots)

def tersoff_total(coords, occupied, gather_index):
    points = jnp.concatenate([coords, occupied], axis=0)
    center = points[:, 1:-1, 1:-1]
    return jnp.sum(cell_energy(center, gather_nearby(points, gather_index)))

def global_forces(state, neighbours):
    padded = jnp.pad(state, ((0, 0), (2, 2), (2, 2), (0, 0)))
    wide = jnp.pad(neighbours, ((0, 0), (1, 1), (1, 1), (0, 0)))
    zero = jnp.zeros((), jnp.int32)

    def one_block(start):
        window = lax.dynamic_slice(padded, (zero, start, zero, zero), (4, CX + 4, NYC + 4, S))
        near_lists = lax.dynamic_slice(wide, (zero, start, zero, zero), (K, CX + 2, NYC + 2, S))
        grads = jax.grad(tersoff_total)(window[:3], window[3:], flat_index(near_lists))
        return -grads[:, 2:-2, 2:-2]
    starts = jnp.arange(N_GX, dtype=jnp.int32) * CX
    blocks = lax.map(one_block, starts)
    return jnp.transpose(blocks, (1, 0, 2, 3, 4)).reshape(3, NXC, NYC, S)

def pack_columns(rows, plan_rows, groups, capacity):
    target = plan_rows[:, 0]
    chosen = (target[:, None] == jnp.arange(groups, dtype=jnp.int32)[None, :]).astype(jnp.int32)
    earlier = jnp.cumsum(chosen, axis=0) - chosen
    place = target * capacity + lax.optimization_barrier(jnp.sum(chosen * earlier, axis=1))
    dispatch = (jnp.arange(groups * capacity, dtype=jnp.int32)[:, None] == place[None, :]).astype(rows.dtype)
    packed = jnp.einsum('rc,acs->ras', dispatch, rows, precision=lax.Precision.HIGHEST)
    return packed.reshape(groups, capacity, rows.shape[0], rows.shape[2])

def reference(displacement, velocity, forces, heights, counts, neighbours, plan):
    along_x = (jnp.arange(NXC, dtype=jnp.int32).astype(jnp.float32) + 0.5) * spacing
    along_y = (jnp.arange(NYC, dtype=jnp.int32).astype(jnp.float32) + 0.5) * spacing
    along_z = (heights.astype(jnp.float32) + 0.5) * spacing
    lattice = jnp.stack([jnp.broadcast_to(along_x[:, None, None], along_z.shape), jnp.broadcast_to(along_y[None, :, None], along_z.shape), along_z])
    occupied = (heights < counts[:, :, None]).astype(jnp.float32)
    offset, speed, force_now = (displacement, velocity, forces)
    for number in range(STEPS):
        speed = speed + half_step * (force_now * force_scale)
        offset = offset + time_step * speed
        state = jnp.concatenate([lattice + offset, occupied[None]], axis=0)
        force_now = global_forces(state, neighbours)
        speed = speed + half_step * (force_now * force_scale)
    rows = jnp.concatenate([offset, speed, occupied[None]], axis=0)
    blocks = rows.reshape(7, N_GX, CX, N_GY, CY, S).transpose(1, 3, 0, 2, 4, 5).reshape(N_GX, N_GY, 7, CX * CY, S)
    packed = jax.vmap(jax.vmap(lambda part_rows, part_plan: pack_columns(part_rows, part_plan, N_GY, CAP)))(blocks, plan)
    return jnp.swapaxes(packed, 1, 2)
```

```python
import functools

import jax
import jax.numpy as jnp
from jax import lax
from jax.experimental import pallas as pl
from jax.experimental.pallas import tpu as pltpu
from jax.sharding import PartitionSpec as P

repulse_a = 1830.8
attract_b = 471.18
decay_one = 2.4799
decay_two = 1.7322
beta_t = 1.1e-06
expo_n = 0.78734
coeff_c2 = 100390.0**2
coeff_d2 = 16.217**2
coeff_h = -0.59825
spacing = 2.4
time_step = 0.001
half_step = 0.0005
force_scale = 9648.53 / 28.0855

FAR = 10000.0
MESH = pl.DeviceIdType.MESH
UNROLL = 4

SIDES = [(dx, dy) for dx in (-1, 0, 1) for dy in (-1, 0, 1) if (dx, dy) != (0, 0)]


def place_of(dx, dy):
    return (dx + 1) * 3 + dy + 1


def near(d):
    return {-1: (0,), 0: (0, 1), 1: (1,)}[d]


LISTS = [(dx, dy, i, j) for dx, dy in SIDES for i in near(dx) for j in near(dy)]


def poly_sin(x):
    y = x * x
    p = -1.0 / 39916800.0
    for c in (1.0 / 362880.0, -1.0 / 5040.0, 1.0 / 120.0, -1.0 / 6.0, 1.0):
        p = p * y + c
    return p * x


def poly_cos(x):
    y = x * x
    p = 1.0 / 479001600.0
    for c in (-1.0 / 3628800.0, 1.0 / 40320.0, -1.0 / 720.0, 1.0 / 24.0, -0.5, 1.0):
        p = p * y + c
    return p


def turn(x, by):
    return pltpu.roll(x, (8 - by) % 8, 0)


def above(value, limit):
    return jnp.where(value > limit, 1.0, jnp.where(value == limit, 0.5, 0.0))


def column_terms(center, near_by):
    occupied = jnp.where(center[2] < 0.5 * FAR, 0.5, 0.0)
    d = [q - p for q, p in zip(near_by, center)]
    square = d[0] * d[0] + d[1] * d[1] + d[2] * d[2]
    clipped = jnp.maximum(square, 1.0)
    inverse = lax.rsqrt(clipped)
    radius = clipped * inverse
    n = [c * inverse for c in d]
    angle = (jnp.clip(radius, 2.7, 3.0) - 2.85) * (0.5 * jnp.pi / 0.15)
    inner, outer = radius < 2.7, radius > 3.0
    w = jnp.where(inner, 1.0, jnp.where(outer, 0.0, 0.5 - 0.5 * poly_sin(angle)))
    slope = jnp.where(inner | outer, 0.0, poly_cos(angle) * (-0.25 * jnp.pi / 0.15))
    turned_n, turned_w, angular, dangular = {}, {}, {}, {}
    zeta = jnp.zeros_like(w)
    for by in (1, 2, 3, 4):
        tn = [turn(c, by) for c in n]
        tw = turn(w, by)
        cosine = n[0] * tn[0] + n[1] * tn[1] + n[2] * tn[2]
        apart = coeff_h - cosine
        spread = apart * apart
        part = 1.0 / (coeff_d2 + spread)
        g = 1.0 + (coeff_c2 / coeff_d2) * spread * part
        zeta = zeta + tw * g
        if by != 4:
            zeta = zeta + turn(w * g, 8 - by)
        turned_n[by], turned_w[by], angular[by] = tn, tw, g
        dangular[by] = (-2.0 * coeff_c2) * apart * (part * part)
    bond = jnp.maximum(zeta, 1.0)
    grown = jnp.exp(expo_n * jnp.log(beta_t * bond))
    order = jnp.exp((-0.5 / expo_n) * jnp.log(1.0 + grown))
    pull = attract_b * jnp.exp(-decay_two * radius)
    push = repulse_a * jnp.exp(-decay_one * radius)
    dzeta = (
        occupied * w * pull * (0.5 * order) * grown / ((1.0 + grown) * bond) * above(zeta, 1.0)
    )
    dw = occupied * (push - pull * order)
    dn = [jnp.zeros_like(w)] * 3
    for by in (1, 2, 3, 4):
        tz = turn(dzeta, by)
        pair = (dzeta * turned_w[by] + tz * w) * dangular[by]
        dw = dw + tz * angular[by]
        for axis in range(3):
            dn[axis] = dn[axis] + pair * turned_n[by][axis]
        if by != 4:
            dw = dw + turn(dzeta * angular[by], 8 - by)
            for axis in range(3):
                dn[axis] = dn[axis] + turn(pair * n[axis], 8 - by)
    dr = occupied * w * (decay_two * pull * order - decay_one * push) + dw * slope
    along = n[0] * dn[0] + n[1] * dn[1] + n[2] * dn[2]
    radial = (dr - along * inverse) * above(square, 1.0)
    return [dn[axis] * inverse + radial * n[axis] for axis in range(3)]


def kernel(
    gx, gy,
    displacement, velocity, forces, heights, counts, neighbours, plan,
    out,
    disp_v, vel_v, for_v, hei_v, nei_v, count_s, plan_s,
    pos, grid_pos, lists, split, terms, speed_v, up, vp, send_u, send_v, got_u, got_v,
    local_sem, pos_send, pos_recv, list_send, list_recv, u_send, u_recv, v_send, v_recv,
):
    a, b = lax.axis_index("gx"), lax.axis_index("gy")

    def at(da, db):
        return lax.rem(a + da + gx, gx), lax.rem(b + db + gy, gy)

    barrier = pltpu.get_barrier_semaphore()
    partners = [at(0, db) for db in range(1, gy)]
    partners += [at(da, db) for da in (-1, 1) for db in (-1, 0, 1)]
    for partner in partners:
        pl.semaphore_signal(barrier, inc=1, device_id=partner, device_id_type=MESH)

    loads = [
        pltpu.make_async_copy(source, target, local_sem.at[number])
        for number, (source, target) in enumerate(
            [
                (displacement, disp_v), (velocity, vel_v), (forces, for_v), (heights, hei_v),
                (neighbours, nei_v), (counts, count_s), (plan, plan_s),
            ]
        )
    ]
    for load in loads:
        load.start()
    for load in loads:
        load.wait()

    for i in range(2):
        high = hei_v[i]
        row = lax.broadcasted_iota(jnp.int32, (2, 128), 0)
        live = high < jnp.where(row == 0, count_s[i, 0], count_s[i, 1])
        occupied = live.astype(jnp.float32)
        for axis in range(3):
            speed = vel_v[axis, i] + half_step * (for_v[axis, i] * force_scale)
            offset = disp_v[axis, i] + time_step * speed
            if axis == 0:
                site = ((2 * a + i).astype(jnp.float32) + 0.5) * spacing
            elif axis == 1:
                site = ((2 * b + row).astype(jnp.float32) + 0.5) * spacing
            else:
                site = (high.astype(jnp.float32) + 0.5) * spacing
            where = site + offset
            if axis == 2:
                where = jnp.where(live, where, where + FAR)
            pos[4, axis * 4 + 2 * i : axis * 4 + 2 * i + 2, :] = where
            for j in range(2):
                speed_v[2 * i + j, axis : axis + 1, :] = speed[j : j + 1]
                up[2 * i + j, axis : axis + 1, :] = offset[j : j + 1]
                up[2 * i + j, axis + 4 : axis + 5, :] = offset[j : j + 1]
        for j in range(2):
            up[2 * i + j, 3:4, :] = occupied[j : j + 1]
            up[2 * i + j, 7:8, :] = occupied[j : j + 1]
            lists[5 + 4 * i + j] = nei_v[:, i, j, :]

    owners = [plan_s[0, 0, c, 0] for c in range(4)]
    place = []
    for c in range(4):
        earlier = jnp.int32(0)
        for e in range(c):
            earlier = earlier + jnp.where(owners[e] == owners[c], 1, 0)
        place.append(owners[c] * 2 + earlier)

    def dealt(rows, half, columns):
        second = (lax.broadcasted_iota(jnp.int32, (rows, 128), 0) >= half).astype(jnp.int32)
        slot = [place[c] - second for c in range(4)]

        def of(owner):
            total = jnp.zeros((rows, 128), jnp.float32)
            for c in range(4):
                total = jnp.where(slot[c] == 2 * owner, columns[c], total)
            return total

        return of

    of_u = dealt(8, 4, [up[c] for c in range(4)])
    for d in range(1, gy):
        send_u[d] = of_u(lax.rem(b + d, gy))
    got_u[b] = of_u(b)

    pl.semaphore_wait(barrier, len(partners))

    copies = []
    for number, (dx, dy) in enumerate(SIDES):
        copies.append(
            pltpu.make_async_remote_copy(
                src_ref=pos.at[4],
                dst_ref=pos.at[place_of(-dx, -dy)],
                send_sem=pos_send.at[number],
                recv_sem=pos_recv.at[number],
                device_id=at(dx, dy),
                device_id_type=MESH,
            )
        )
    for number, (dx, dy, i, j) in enumerate(LISTS):
        x, y = 1 + i - 2 * dx, 1 + j - 2 * dy
        copies.append(
            pltpu.make_async_remote_copy(
                src_ref=lists.at[5 + 4 * i + j],
                dst_ref=lists.at[4 * x + y],
                send_sem=list_send.at[number],
                recv_sem=list_recv.at[number],
                device_id=at(dx, dy),
                device_id_type=MESH,
            )
        )
    for copy in copies:
        copy.start()
    u_copies = []
    for d in range(1, gy):
        u_copies.append(
            pltpu.make_async_remote_copy(
                src_ref=send_u.at[d],
                dst_ref=got_u.at[b],
                send_sem=u_send.at[d],
                recv_sem=u_recv.at[d],
                device_id=at(0, d),
                device_id_type=MESH,
            )
        )
    for copy in u_copies:
        copy.start()
    for copy in copies:
        copy.wait_recv()

    for dx in (-1, 0, 1):
        for dy in (-1, 0, 1):
            gone = ((a + dx) < 0) | ((a + dx) >= gx) | ((b + dy) < 0) | ((b + dy) >= gy)
            lift = jnp.where(gone, FAR, 0.0)
            for axis in range(3):
                for i in range(2):
                    first = axis * 36 + (2 * dx + 2 + i) * 6 + 2 * dy + 2
                    rows = pos[place_of(dx, dy), axis * 4 + 2 * i : axis * 4 + 2 * i + 2, :]
                    grid_pos[first : first + 2, :] = rows + lift if axis == 2 else rows

    rows16 = [
        (lax.broadcasted_iota(jnp.int32, (16, 128), 0) + 16 * k).astype(jnp.float32).astype(jnp.bfloat16)
        for k in range(8)
    ]
    one, none = jnp.ones((16, 128), jnp.bfloat16), jnp.zeros((16, 128), jnp.bfloat16)

    def column(k, part, total):
        x, y = 1 + k // 4, 1 + k % 4
        base = (x - 1) * 6 + y - 1
        entries = lists[k]
        slot, offset = entries & 127, entries >> 7
        near_by = [None] * 3
        for c in range(9):
            here = base + (c // 3) * 6 + c % 3
            for axis in range(3):
                source = jnp.broadcast_to(grid_pos[pl.ds(axis * 36 + here, 1), :], (8, 128))
                taken = jnp.take_along_axis(source, slot, axis=1)
                near_by[axis] = taken if c == 0 else jnp.where(offset == c, taken, near_by[axis])
        center = [
            jnp.broadcast_to(grid_pos[pl.ds(axis * 36 + base + 7, 1), :], (8, 128)) for axis in range(3)
        ]
        grads = column_terms(center, near_by)
        for axis in range(3):
            terms[k, axis] = grads[axis]
        highs = [g.astype(jnp.bfloat16).astype(jnp.float32) for g in grads]
        lows = [g - h for g, h in zip(grads, highs)]
        for t in range(4):
            cx, cy = 3 + t // 2 - x, 3 + t % 2 - y
            inside = (cx >= 0) & (cx <= 2) & (cy >= 0) & (cy <= 2)
            hit = offset == jnp.where(inside, 3 * cx + cy, -1)
            for axis in range(3):
                row = part * 192 + (t * 3 + axis) * 8
                split[pl.ds(row, 8), :] = jnp.where(hit, highs[axis], 0.0)
                split[pl.ds(row + 96, 8), :] = jnp.where(hit, lows[axis], 0.0)
        slot_f = slot.astype(jnp.float32)
        for m in range(0, 8, 2):
            left, right = [], []
            for e in (m, m + 1):
                left.append(split[pl.ds(part * 192 + e, 24, stride=8), :].astype(jnp.bfloat16))
                wanted = jnp.broadcast_to(slot_f[e : e + 1], (16, 128)).astype(jnp.bfloat16)
                right.append(
                    jnp.concatenate([jnp.where(r == wanted, one, none) for r in rows16], axis=0)
                )
            total = total + lax.dot_general(
                jnp.concatenate(left, axis=1),
                jnp.concatenate(right, axis=1),
                (((1,), (1,)), ((), ())),
                preferred_element_type=jnp.float32,
            )
        return total

    def some_columns(step, total):
        for part in range(UNROLL):
            total = column(step * UNROLL + part, part, total)
        return total

    total = lax.fori_loop(0, 16 // UNROLL, some_columns, jnp.zeros((24, 128), jnp.float32))
    on_neighbours = total[0:12] + total[12:24]

    for t in range(4):
        own = 5 + 4 * (t // 2) + t % 2
        for axis in range(3):
            force = jnp.sum(terms[own, axis], axis=0, keepdims=True)
            force = force - on_neighbours[t * 3 + axis : t * 3 + axis + 1]
            speed = speed_v[t, axis : axis + 1, :] + half_step * (force * force_scale)
            vp[t, axis : axis + 1, :] = speed
            vp[t, axis + 3 : axis + 4, :] = speed
    of_v = dealt(6, 3, [vp[c] for c in range(4)])
    v_copies = []
    for d in range(1, gy):
        send_v[d] = of_v(lax.rem(b + d, gy))
        v_copies.append(
            pltpu.make_async_remote_copy(
                src_ref=send_v.at[d],
                dst_ref=got_v.at[b],
                send_sem=v_send.at[d],
                recv_sem=v_recv.at[d],
                device_id=at(0, d),
                device_id_type=MESH,
            )
        )
    for copy in v_copies:
        copy.start()
    got_v[b] = of_v(b)
    for copy in u_copies:
        copy.wait_recv()
    for o in range(gy):
        for s in range(2):
            out[0, 0, o, s, 0:3, :] = got_u[o, 4 * s : 4 * s + 3, :]
            out[0, 0, o, s, 6:7, :] = got_u[o, 4 * s + 3 : 4 * s + 4, :]
    for copy in v_copies:
        copy.wait_recv()
    for o in range(gy):
        for s in range(2):
            out[0, 0, o, s, 3:6, :] = got_v[o, 3 * s : 3 * s + 3, :]
    for copy in copies + u_copies + v_copies:
        copy.wait_send()


def per_device(gx, gy, displacement, velocity, forces, heights, counts, neighbours, plan):
    dma = pltpu.SemaphoreType.DMA
    f32 = jnp.float32
    anywhere = pl.BlockSpec(memory_space=pl.ANY)
    return pl.pallas_call(
        functools.partial(kernel, gx, gy),
        out_shape=jax.ShapeDtypeStruct((1, 1, gy, 2, 7, 128), f32),
        in_specs=[anywhere] * 7,
        out_specs=pl.BlockSpec(memory_space=pltpu.VMEM),
        scratch_shapes=[
            pltpu.VMEM((3, 2, 2, 128), f32),
            pltpu.VMEM((3, 2, 2, 128), f32),
            pltpu.VMEM((3, 2, 2, 128), f32),
            pltpu.VMEM((2, 2, 128), jnp.int32),
            pltpu.VMEM((8, 2, 2, 128), jnp.int32),
            pltpu.SMEM((2, 2), jnp.int32),
            pltpu.SMEM((1, 1, 4, 1), jnp.int32),
            pltpu.VMEM((9, 16, 128), f32),
            pltpu.VMEM((112, 128), f32),
            pltpu.VMEM((16, 8, 128), jnp.int32),
            pltpu.VMEM((UNROLL * 192, 128), f32),
            pltpu.VMEM((16, 3, 8, 128), f32),
            pltpu.VMEM((4, 8, 128), f32),
            pltpu.VMEM((4, 8, 128), f32),
            pltpu.VMEM((4, 6, 128), f32),
            pltpu.VMEM((gy, 8, 128), f32),
            pltpu.VMEM((gy, 6, 128), f32),
            pltpu.VMEM((gy, 8, 128), f32),
            pltpu.VMEM((gy, 6, 128), f32),
            dma((7,)),
            dma((len(SIDES),)),
            dma((len(SIDES),)),
            dma((len(LISTS),)),
            dma((len(LISTS),)),
            dma((gy,)),
            dma((gy,)),
            dma((gy,)),
            dma((gy,)),
        ],
        compiler_params=pltpu.CompilerParams(collective_id=0, has_side_effects=True),
        name="verlet_recut",
    )(displacement, velocity, forces, heights, counts, neighbours, plan)


def solution(mesh):
    in_specs = (
        P(None, "gx", "gy", None),
        P(None, "gx", "gy", None),
        P(None, "gx", "gy", None),
        P("gx", "gy", None),
        P("gx", "gy"),
        P(None, "gx", "gy", None),
        P("gx", "gy", None, None),
    )
    out_specs = P("gx", "gy", None, None, None, None)
    gx, gy = mesh.shape["gx"], mesh.shape["gy"]
    return jax.shard_map(
        functools.partial(per_device, gx, gy),
        mesh=mesh, in_specs=in_specs, out_specs=out_specs, check_vma=False,
    )
```

```python
import functools

import jax
import jax.numpy as jnp
from jax import lax
from jax.experimental import pallas as pl
from jax.experimental.pallas import tpu as pltpu
from jax.sharding import PartitionSpec as P

repulse_a = 1830.8
attract_b = 471.18
decay_one = 2.4799
decay_two = 1.7322
beta_t = 1.1e-06
expo_n = 0.78734
coeff_c2 = 100390.0**2
coeff_d2 = 16.217**2
coeff_h = -0.59825
spacing = 2.4
time_step = 0.001
half_step = 0.0005
force_scale = 9648.53 / 28.0855

FAR = 10000.0
MESH = pl.DeviceIdType.MESH
UNROLL = 4
REACH = 4
VMEM_LIMIT = 8 * 1024 * 1024

SIDES = [(dx, dy) for dx in (-1, 0, 1) for dy in (-1, 0, 1) if (dx, dy) != (0, 0)]


def place_of(dx, dy):
    return (dx + 1) * 3 + dy + 1


def near(d):
    return {-1: (0,), 0: (0, 1), 1: (1,)}[d]


LISTS = [(dx, dy, i, j) for dx, dy in SIDES for i in near(dx) for j in near(dy)]


def poly_sin(x):
    y = x * x
    p = -1.0 / 39916800.0
    for c in (1.0 / 362880.0, -1.0 / 5040.0, 1.0 / 120.0, -1.0 / 6.0, 1.0):
        p = p * y + c
    return p * x


def poly_cos(x):
    y = x * x
    p = 1.0 / 479001600.0
    for c in (-1.0 / 3628800.0, 1.0 / 40320.0, -1.0 / 720.0, 1.0 / 24.0, -0.5, 1.0):
        p = p * y + c
    return p


def turn(x, by):
    return pltpu.roll(x, (8 - by) % 8, 0)


def above(value, limit):
    return jnp.where(value > limit, 1.0, jnp.where(value == limit, 0.5, 0.0))


def column_terms(center, near_by):
    occupied = jnp.where(center[2] < 0.5 * FAR, 0.5, 0.0)
    d = [q - p for q, p in zip(near_by, center)]
    square = d[0] * d[0] + d[1] * d[1] + d[2] * d[2]
    clipped = jnp.maximum(square, 1.0)
    inverse = lax.rsqrt(clipped)
    radius = clipped * inverse
    n = [c * inverse for c in d]
    angle = (jnp.clip(radius, 2.7, 3.0) - 2.85) * (0.5 * jnp.pi / 0.15)
    inner, outer = radius < 2.7, radius > 3.0
    w = jnp.where(inner, 1.0, jnp.where(outer, 0.0, 0.5 - 0.5 * poly_sin(angle)))
    slope = jnp.where(inner | outer, 0.0, poly_cos(angle) * (-0.25 * jnp.pi / 0.15))
    turned_n, turned_w, angular, dangular = {}, {}, {}, {}
    zeta = jnp.zeros_like(w)
    for by in (1, 2, 3, 4):
        tn = [turn(c, by) for c in n]
        tw = turn(w, by)
        cosine = n[0] * tn[0] + n[1] * tn[1] + n[2] * tn[2]
        apart = coeff_h - cosine
        spread = apart * apart
        part = 1.0 / (coeff_d2 + spread)
        g = 1.0 + (coeff_c2 / coeff_d2) * spread * part
        zeta = zeta + tw * g
        if by != 4:
            zeta = zeta + turn(w * g, 8 - by)
        turned_n[by], turned_w[by], angular[by] = tn, tw, g
        dangular[by] = (-2.0 * coeff_c2) * apart * (part * part)
    bond = jnp.maximum(zeta, 1.0)
    grown = jnp.exp(expo_n * jnp.log(beta_t * bond))
    order = jnp.exp((-0.5 / expo_n) * jnp.log(1.0 + grown))
    pull = attract_b * jnp.exp(-decay_two * radius)
    push = repulse_a * jnp.exp(-decay_one * radius)
    dzeta = (
        occupied * w * pull * (0.5 * order) * grown / ((1.0 + grown) * bond) * above(zeta, 1.0)
    )
    dw = occupied * (push - pull * order)
    dn = [jnp.zeros_like(w)] * 3
    for by in (1, 2, 3, 4):
        tz = turn(dzeta, by)
        pair = (dzeta * turned_w[by] + tz * w) * dangular[by]
        dw = dw + tz * angular[by]
        for axis in range(3):
            dn[axis] = dn[axis] + pair * turned_n[by][axis]
        if by != 4:
            dw = dw + turn(dzeta * angular[by], 8 - by)
            for axis in range(3):
                dn[axis] = dn[axis] + turn(pair * n[axis], 8 - by)
    dr = occupied * w * (decay_two * pull * order - decay_one * push) + dw * slope
    along = n[0] * dn[0] + n[1] * dn[1] + n[2] * dn[2]
    radial = (dr - along * inverse) * above(square, 1.0)
    return [dn[axis] * inverse + radial * n[axis] for axis in range(3)]


def kernel(
    gx, gy,
    displacement, velocity, forces, heights, counts, neighbours, plan,
    out,
    disp_v, vel_v, for_v, hei_v, nei_v, count_s, plan_s,
    pos, grid_pos, lists, split, terms, speed_v, up, vp, send_u, send_v, got_u, got_v,
    local_sem, pos_send, pos_recv, list_send, list_recv, u_send, u_recv, v_send, v_recv, ring,
):
    a, b = lax.axis_index("gx"), lax.axis_index("gy")

    def at(da, db):
        return lax.rem(a + da + gx, gx), lax.rem(b + db + gy, gy)

    barrier = pltpu.get_barrier_semaphore()
    greeted = [d for d in range(1, gy) if min(d, gy - d) <= REACH]
    partners = [at(0, d) for d in greeted]
    partners += [at(da, db) for da in (-1, 1) for db in (-1, 0, 1)]
    for partner in partners:
        pl.semaphore_signal(barrier, inc=1, device_id=partner, device_id_type=MESH)

    loads = [
        pltpu.make_async_copy(source, target, local_sem.at[number])
        for number, (source, target) in enumerate(
            [
                (displacement, disp_v), (velocity, vel_v), (forces, for_v), (heights, hei_v),
                (neighbours, nei_v), (counts, count_s), (plan, plan_s),
            ]
        )
    ]
    for load in loads:
        load.start()
    for load in loads:
        load.wait()

    for i in range(2):
        high = hei_v[i]
        row = lax.broadcasted_iota(jnp.int32, (2, 128), 0)
        live = high < jnp.where(row == 0, count_s[i, 0], count_s[i, 1])
        occupied = live.astype(jnp.float32)
        for axis in range(3):
            speed = vel_v[axis, i] + half_step * (for_v[axis, i] * force_scale)
            offset = disp_v[axis, i] + time_step * speed
            if axis == 0:
                site = ((2 * a + i).astype(jnp.float32) + 0.5) * spacing
            elif axis == 1:
                site = ((2 * b + row).astype(jnp.float32) + 0.5) * spacing
            else:
                site = (high.astype(jnp.float32) + 0.5) * spacing
            where = site + offset
            if axis == 2:
                where = jnp.where(live, where, where + FAR)
            pos[4, axis, 2 * i : 2 * i + 2, :] = where
            for j in range(2):
                speed_v[2 * i + j, axis : axis + 1, :] = speed[j : j + 1]
                up[2 * i + j, 2 * axis : 2 * axis + 2, :] = jnp.broadcast_to(offset[j : j + 1], (2, 128))
        for j in range(2):
            up[2 * i + j, 6:8, :] = jnp.broadcast_to(occupied[j : j + 1], (2, 128))
            lists[5 + 4 * i + j] = nei_v[:, i, j, :]

    pl.semaphore_wait(barrier, len(partners))

    copies = []
    for number, (dx, dy) in enumerate(SIDES):
        copies.append(
            pltpu.make_async_remote_copy(
                src_ref=pos.at[4],
                dst_ref=pos.at[place_of(-dx, -dy)],
                send_sem=pos_send.at[number],
                recv_sem=pos_recv.at[number],
                device_id=at(dx, dy),
                device_id_type=MESH,
            )
        )
    for number, (dx, dy, i, j) in enumerate(LISTS):
        x, y = 1 + i - 2 * dx, 1 + j - 2 * dy
        copies.append(
            pltpu.make_async_remote_copy(
                src_ref=lists.at[5 + 4 * i + j],
                dst_ref=lists.at[4 * x + y],
                send_sem=list_send.at[number],
                recv_sem=list_recv.at[number],
                device_id=at(dx, dy),
                device_id_type=MESH,
            )
        )
    for copy in copies:
        copy.start()
    owners = [plan_s[0, 0, 0, c] for c in range(4)]
    place = []
    for c in range(4):
        earlier = jnp.int32(0)
        for e in range(c):
            earlier = earlier + jnp.where(owners[e] == owners[c], 1, 0)
        place.append(owners[c] * 2 + earlier)

    def dealt(rows, columns):
        second = lax.broadcasted_iota(jnp.int32, (rows, 128), 0) & 1
        slot = [place[c] - second for c in range(4)]

        def of(owner):
            total = jnp.zeros((rows, 128), jnp.float32)
            for c in range(4):
                total = jnp.where(slot[c] == 2 * owner, columns[c], total)
            return total

        return of

    of_u = dealt(8, [up[c] for c in range(4)])
    for d in range(1, gy):
        send_u[d] = of_u(lax.rem(b + d, gy))
    got_u[b] = of_u(b)

    u_copies = {}
    for d in range(1, gy):
        u_copies[d] = pltpu.make_async_remote_copy(
            src_ref=send_u.at[d],
            dst_ref=got_u.at[b],
            send_sem=u_send.at[d],
            recv_sem=u_recv.at[d],
            device_id=at(0, d),
            device_id_type=MESH,
        )
    for copy in copies:
        copy.wait_recv()
    known = [d for d in range(1, gy) if min(d, gy - d) <= REACH + 1]
    for d in known:
        u_copies[d].start()
    for d in (1, gy - 1):
        pl.semaphore_signal(ring, inc=1, device_id=at(0, d), device_id_type=MESH)

    for dx in (-1, 0, 1):
        for dy in (-1, 0, 1):
            gone = ((a + dx) < 0) | ((a + dx) >= gx) | ((b + dy) < 0) | ((b + dy) >= gy)
            lift = jnp.where(gone, FAR, 0.0)
            for axis in range(3):
                for i in range(2):
                    first = axis * 36 + (2 * dx + 2 + i) * 6 + 2 * dy + 2
                    rows = pos[place_of(dx, dy), axis, 2 * i : 2 * i + 2, :]
                    grid_pos[first : first + 2, :] = rows + lift if axis == 2 else rows

    rows16 = [
        (lax.broadcasted_iota(jnp.int32, (16, 128), 0) + 16 * k).astype(jnp.float32).astype(jnp.bfloat16)
        for k in range(8)
    ]
    one, none = jnp.ones((16, 128), jnp.bfloat16), jnp.zeros((16, 128), jnp.bfloat16)

    def column(k, part, total):
        x, y = 1 + k // 4, 1 + k % 4
        base = (x - 1) * 6 + y - 1
        entries = lists[k]
        slot, offset = entries & 127, entries >> 7
        near_by = [None] * 3
        for c in range(9):
            here = base + (c // 3) * 6 + c % 3
            for axis in range(3):
                source = jnp.broadcast_to(grid_pos[pl.ds(axis * 36 + here, 1), :], (8, 128))
                taken = jnp.take_along_axis(source, slot, axis=1)
                near_by[axis] = taken if c == 0 else jnp.where(offset == c, taken, near_by[axis])
        center = [
            jnp.broadcast_to(grid_pos[pl.ds(axis * 36 + base + 7, 1), :], (8, 128)) for axis in range(3)
        ]
        grads = column_terms(center, near_by)
        for axis in range(3):
            terms[k, axis] = grads[axis]
        highs = [g.astype(jnp.bfloat16).astype(jnp.float32) for g in grads]
        lows = [g - h for g, h in zip(grads, highs)]
        for t in range(4):
            cx, cy = 3 + t // 2 - x, 3 + t % 2 - y
            inside = (cx >= 0) & (cx <= 2) & (cy >= 0) & (cy <= 2)
            hit = offset == jnp.where(inside, 3 * cx + cy, -1)
            for axis in range(3):
                row = part * 192 + (t * 3 + axis) * 8
                split[pl.ds(row, 8), :] = jnp.where(hit, highs[axis], 0.0)
                split[pl.ds(row + 96, 8), :] = jnp.where(hit, lows[axis], 0.0)
        slot_f = slot.astype(jnp.float32)
        for m in range(0, 8, 2):
            left, right = [], []
            for e in (m, m + 1):
                left.append(split[pl.ds(part * 192 + e, 24, stride=8), :].astype(jnp.bfloat16))
                wanted = jnp.broadcast_to(slot_f[e : e + 1], (16, 128)).astype(jnp.bfloat16)
                right.append(
                    jnp.concatenate([jnp.where(r == wanted, one, none) for r in rows16], axis=0)
                )
            total = total + lax.dot_general(
                jnp.concatenate(left, axis=1),
                jnp.concatenate(right, axis=1),
                (((1,), (1,)), ((), ())),
                preferred_element_type=jnp.float32,
            )
        return total

    def some_columns(step, total):
        for part in range(UNROLL):
            total = column(step * UNROLL + part, part, total)
        return total

    total = lax.fori_loop(0, 16 // UNROLL, some_columns, jnp.zeros((24, 128), jnp.float32))
    pl.semaphore_wait(ring, 2)
    for d in range(1, gy):
        if d not in known:
            u_copies[d].start()
    on_neighbours = total[0:12] + total[12:24]

    for t in range(4):
        own = 5 + 4 * (t // 2) + t % 2
        for axis in range(3):
            force = jnp.sum(terms[own, axis], axis=0, keepdims=True)
            force = force - on_neighbours[t * 3 + axis : t * 3 + axis + 1]
            speed = speed_v[t, axis : axis + 1, :] + half_step * (force * force_scale)
            vp[t, 2 * axis : 2 * axis + 2, :] = jnp.broadcast_to(speed, (2, 128))
    of_v = dealt(6, [vp[c] for c in range(4)])
    v_copies = []
    for d in sorted(range(1, gy), key=lambda d: -min(d, gy - d)):
        send_v[d] = of_v(lax.rem(b + d, gy))
        copy = pltpu.make_async_remote_copy(
            src_ref=send_v.at[d],
            dst_ref=got_v.at[b],
            send_sem=v_send.at[d],
            recv_sem=v_recv.at[d],
            device_id=at(0, d),
            device_id_type=MESH,
        )
        copy.start()
        v_copies.append(copy)
    got_v[b] = of_v(b)
    for copy in u_copies.values():
        copy.wait_recv()
    for o in range(gy):
        for r in range(4):
            out[0, 0, o, (0, 1, 2, 6)[r], :, :] = got_u[o, 2 * r : 2 * r + 2, :]
    for copy in v_copies:
        copy.wait_recv()
    for o in range(gy):
        for r in range(3):
            out[0, 0, o, r + 3, :, :] = got_v[o, 2 * r : 2 * r + 2, :]
    for copy in copies + list(u_copies.values()) + v_copies:
        copy.wait_send()


def per_device(gx, gy, displacement, velocity, forces, heights, counts, neighbours, plan):
    dma = pltpu.SemaphoreType.DMA
    f32 = jnp.float32
    anywhere = pl.BlockSpec(memory_space=pltpu.HBM)
    inputs = [displacement, velocity, forces, heights, counts, neighbours, jnp.swapaxes(plan, 2, 3)]
    inputs = [pltpu.with_memory_space_constraint(value, pltpu.HBM) for value in inputs]
    arrived = pl.pallas_call(
        functools.partial(kernel, gx, gy),
        out_shape=jax.ShapeDtypeStruct((1, 1, gy, 7, 2, 128), f32),
        in_specs=[anywhere] * 7,
        out_specs=pl.BlockSpec(memory_space=pltpu.VMEM),
        scratch_shapes=[
            pltpu.VMEM((3, 2, 2, 128), f32),
            pltpu.VMEM((3, 2, 2, 128), f32),
            pltpu.VMEM((3, 2, 2, 128), f32),
            pltpu.VMEM((2, 2, 128), jnp.int32),
            pltpu.VMEM((8, 2, 2, 128), jnp.int32),
            pltpu.SMEM((2, 2), jnp.int32),
            pltpu.SMEM((1, 1, 1, 4), jnp.int32),
            pltpu.VMEM((9, 3, 4, 128), f32),
            pltpu.VMEM((112, 128), f32),
            pltpu.VMEM((16, 8, 128), jnp.int32),
            pltpu.VMEM((UNROLL * 192, 128), f32),
            pltpu.VMEM((16, 3, 8, 128), f32),
            pltpu.VMEM((4, 8, 128), f32),
            pltpu.VMEM((4, 8, 128), f32),
            pltpu.VMEM((4, 6, 128), f32),
            pltpu.VMEM((gy, 8, 128), f32),
            pltpu.VMEM((gy, 6, 128), f32),
            pltpu.VMEM((gy, 8, 128), f32),
            pltpu.VMEM((gy, 6, 128), f32),
            dma((7,)),
            dma((len(SIDES),)),
            dma((len(SIDES),)),
            dma((len(LISTS),)),
            dma((len(LISTS),)),
            dma((gy,)),
            dma((gy,)),
            dma((gy,)),
            dma((gy,)),
            pltpu.SemaphoreType.REGULAR,
        ],
        compiler_params=pltpu.CompilerParams(
            collective_id=0, has_side_effects=True, vmem_limit_bytes=VMEM_LIMIT
        ),
        name="verlet_recut",
    )(*inputs)
    return jnp.swapaxes(arrived, 3, 4)


def solution(mesh):
    in_specs = (
        P(None, "gx", "gy", None),
        P(None, "gx", "gy", None),
        P(None, "gx", "gy", None),
        P("gx", "gy", None),
        P("gx", "gy"),
        P(None, "gx", "gy", None),
        P("gx", "gy", None, None),
    )
    out_specs = P("gx", "gy", None, None, None, None)
    gx, gy = mesh.shape["gx"], mesh.shape["gy"]
    return jax.shard_map(
        functools.partial(per_device, gx, gy),
        mesh=mesh, in_specs=in_specs, out_specs=out_specs, check_vma=False,
    )
```

```python
import functools

import jax
import jax.numpy as jnp
from jax import lax
from jax.experimental import pallas as pl
from jax.experimental.pallas import tpu as pltpu
from jax.sharding import PartitionSpec as P

repulse_a = 1830.8
attract_b = 471.18
decay_one = 2.4799
decay_two = 1.7322
beta_t = 1.1e-06
expo_n = 0.78734
coeff_c2 = 100390.0**2
coeff_d2 = 16.217**2
coeff_h = -0.59825
spacing = 2.4
time_step = 0.001
half_step = 0.0005
force_scale = 9648.53 / 28.0855

FAR = 10000.0
MESH = pl.DeviceIdType.MESH
UNROLL = 4
VMEM_LIMIT = 8 * 1024 * 1024

SIDES = [(dx, dy) for dx in (-1, 0, 1) for dy in (-1, 0, 1) if (dx, dy) != (0, 0)]


CORNERS_FIRST = sorted(SIDES, key=lambda side: -abs(side[0]) - abs(side[1]))


def place_of(dx, dy):
    return (dx + 1) * 3 + dy + 1


def near(d):
    return {-1: (0,), 0: (0, 1), 1: (1,)}[d]


LISTS = [(dx, dy, i, j) for dx, dy in SIDES for i in near(dx) for j in near(dy)]


def poly_sin(x):
    y = x * x
    p = -1.0 / 39916800.0
    for c in (1.0 / 362880.0, -1.0 / 5040.0, 1.0 / 120.0, -1.0 / 6.0, 1.0):
        p = p * y + c
    return p * x


def poly_cos(x):
    y = x * x
    p = 1.0 / 479001600.0
    for c in (-1.0 / 3628800.0, 1.0 / 40320.0, -1.0 / 720.0, 1.0 / 24.0, -0.5, 1.0):
        p = p * y + c
    return p


def turn(x, by):
    return pltpu.roll(x, (8 - by) % 8, 0)


def above(value, limit):
    return jnp.where(value > limit, 1.0, jnp.where(value == limit, 0.5, 0.0))


def column_terms(center, near_by):
    occupied = jnp.where(center[2] < 0.5 * FAR, 0.5, 0.0)
    d = [q - p for q, p in zip(near_by, center)]
    square = d[0] * d[0] + d[1] * d[1] + d[2] * d[2]
    clipped = jnp.maximum(square, 1.0)
    inverse = lax.rsqrt(clipped)
    radius = clipped * inverse
    n = [c * inverse for c in d]
    angle = (jnp.clip(radius, 2.7, 3.0) - 2.85) * (0.5 * jnp.pi / 0.15)
    inner, outer = radius < 2.7, radius > 3.0
    w = jnp.where(inner, 1.0, jnp.where(outer, 0.0, 0.5 - 0.5 * poly_sin(angle)))
    slope = jnp.where(inner | outer, 0.0, poly_cos(angle) * (-0.25 * jnp.pi / 0.15))
    turned_n, turned_w, angular, dangular = {}, {}, {}, {}
    zeta = jnp.zeros_like(w)
    for by in (1, 2, 3, 4):
        tn = [turn(c, by) for c in n]
        tw = turn(w, by)
        cosine = n[0] * tn[0] + n[1] * tn[1] + n[2] * tn[2]
        apart = coeff_h - cosine
        spread = apart * apart
        part = 1.0 / (coeff_d2 + spread)
        g = 1.0 + (coeff_c2 / coeff_d2) * spread * part
        zeta = zeta + tw * g
        if by != 4:
            zeta = zeta + turn(w * g, 8 - by)
        turned_n[by], turned_w[by], angular[by] = tn, tw, g
        dangular[by] = (-2.0 * coeff_c2) * apart * (part * part)
    bond = jnp.maximum(zeta, 1.0)
    grown = jnp.exp(expo_n * jnp.log(beta_t * bond))
    order = jnp.exp((-0.5 / expo_n) * jnp.log(1.0 + grown))
    pull = attract_b * jnp.exp(-decay_two * radius)
    push = repulse_a * jnp.exp(-decay_one * radius)
    dzeta = (
        occupied * w * pull * (0.5 * order) * grown / ((1.0 + grown) * bond) * above(zeta, 1.0)
    )
    dw = occupied * (push - pull * order)
    dn = [jnp.zeros_like(w)] * 3
    for by in (1, 2, 3, 4):
        tz = turn(dzeta, by)
        pair = (dzeta * turned_w[by] + tz * w) * dangular[by]
        dw = dw + tz * angular[by]
        for axis in range(3):
            dn[axis] = dn[axis] + pair * turned_n[by][axis]
        if by != 4:
            dw = dw + turn(dzeta * angular[by], 8 - by)
            for axis in range(3):
                dn[axis] = dn[axis] + turn(pair * n[axis], 8 - by)
    dr = occupied * w * (decay_two * pull * order - decay_one * push) + dw * slope
    along = n[0] * dn[0] + n[1] * dn[1] + n[2] * dn[2]
    radial = (dr - along * inverse) * above(square, 1.0)
    return [dn[axis] * inverse + radial * n[axis] for axis in range(3)]


def kernel(
    gx, gy,
    displacement, velocity, forces, heights, counts, neighbours, plan,
    out,
    disp_v, vel_v, for_v, hei_v, nei_v, count_s, plan_s,
    pos, grid_pos, lists, split, terms, speed_v, up, vp, send_u, send_v, got_u, got_v,
    local_sem, pos_send, pos_recv, list_send, list_recv, u_send, u_recv, v_send, v_recv, known,
):
    a, b = lax.axis_index("gx"), lax.axis_index("gy")

    def at(da, db):
        return a + da, b + db

    def there(da, db):
        tests = {-1: a > 0, 0: None, 1: a < gx - 1}[da], {-1: b > 0, 0: None, 1: b < gy - 1}[db]
        tests = [t for t in tests if t is not None]
        return tests[0] if len(tests) == 1 else tests[0] & tests[1]

    barrier = pltpu.get_barrier_semaphore()
    def around(d):
        return a, lax.rem(b + d + gy, gy)

    for dx, dy in CORNERS_FIRST:
        if dx != 0:

            @pl.when(there(dx, dy))
            def _():
                pl.semaphore_signal(barrier, inc=1, device_id=at(dx, dy), device_id_type=MESH)

    pl.semaphore_signal(barrier, inc=1, device_id=around(-1), device_id_type=MESH)

    @pl.when(b < gy - 1)
    def _():
        pl.semaphore_signal(barrier, inc=1, device_id=around(1), device_id_type=MESH)

    loads = [
        pltpu.make_async_copy(source, target, local_sem.at[number])
        for number, (source, target) in enumerate(
            [
                (displacement, disp_v), (velocity, vel_v), (forces, for_v), (heights, hei_v),
                (neighbours, nei_v), (counts, count_s), (plan, plan_s),
            ]
        )
    ]
    for load in loads:
        load.start()
    for load in loads:
        load.wait()

    for i in range(2):
        high = hei_v[i]
        row = lax.broadcasted_iota(jnp.int32, (2, 128), 0)
        live = high < jnp.where(row == 0, count_s[i, 0], count_s[i, 1])
        occupied = live.astype(jnp.float32)
        for axis in range(3):
            speed = vel_v[axis, i] + half_step * (for_v[axis, i] * force_scale)
            offset = disp_v[axis, i] + time_step * speed
            if axis == 0:
                site = ((2 * a + i).astype(jnp.float32) + 0.5) * spacing
            elif axis == 1:
                site = ((2 * b + row).astype(jnp.float32) + 0.5) * spacing
            else:
                site = (high.astype(jnp.float32) + 0.5) * spacing
            where = site + offset
            if axis == 2:
                where = jnp.where(live, where, where + FAR)
            pos[4, axis, 2 * i : 2 * i + 2, :] = where
            for j in range(2):
                speed_v[2 * i + j, axis : axis + 1, :] = speed[j : j + 1]
                up[2 * i + j, 2 * axis : 2 * axis + 2, :] = jnp.broadcast_to(offset[j : j + 1], (2, 128))
        for j in range(2):
            up[2 * i + j, 6:8, :] = jnp.broadcast_to(occupied[j : j + 1], (2, 128))
            lists[5 + 4 * i + j] = nei_v[:, i, j, :]

    wide = (a > 0).astype(jnp.int32) + (a < gx - 1).astype(jnp.int32)
    high = 1 + (b > 0).astype(jnp.int32) + (b < gy - 1).astype(jnp.int32)
    pl.semaphore_wait(barrier, wide * high + 1 + (b > 0).astype(jnp.int32))

    copies = {side: [] for side in SIDES}
    for number, (dx, dy) in enumerate(SIDES):
        copies[dx, dy].append(
            pltpu.make_async_remote_copy(
                src_ref=pos.at[4],
                dst_ref=pos.at[place_of(-dx, -dy)],
                send_sem=pos_send.at[number],
                recv_sem=pos_recv.at[number],
                device_id=at(dx, dy),
                device_id_type=MESH,
            )
        )
    for number, (dx, dy, i, j) in enumerate(LISTS):
        x, y = 1 + i - 2 * dx, 1 + j - 2 * dy
        copies[dx, dy].append(
            pltpu.make_async_remote_copy(
                src_ref=lists.at[5 + 4 * i + j],
                dst_ref=lists.at[4 * x + y],
                send_sem=list_send.at[number],
                recv_sem=list_recv.at[number],
                device_id=at(dx, dy),
                device_id_type=MESH,
            )
        )
    for dx, dy in CORNERS_FIRST:

        @pl.when(there(dx, dy))
        def _():
            for copy in copies[dx, dy]:
                copy.start()

        @pl.when(jnp.logical_not(there(dx, dy)))
        def _():
            for i in near(-dx):
                for j in near(-dy):
                    lists[4 * (1 + i + 2 * dx) + 1 + j + 2 * dy] = jnp.zeros((8, 128), jnp.int32)

    half = min(2 * gy // 3, gy - 2)

    def tell(number, target):
        pl.semaphore_signal(known.at[number], inc=1, device_id=(a, target), device_id_type=MESH)

    @pl.when(b >= 3)
    def _():
        pl.semaphore_wait(known.at[0], 1)

    @pl.when((b >= 2) & (b < gy - 1))
    def _():
        tell(0, b + 1)

    @pl.when(b == gy - 1)
    def _():
        for o in range(gy - 1):
            tell(2, o)

    @pl.when((b >= 2) & (b <= half))
    def _():
        pl.semaphore_wait(known.at[1], 1)

    @pl.when((b >= 1) & (b < half))
    def _():
        tell(1, b + 1)

    waits_for_last = (b > half) & (b < gy - 1)

    owners = [plan_s[0, 0, 0, c] for c in range(4)]
    place = []
    for c in range(4):
        earlier = jnp.int32(0)
        for e in range(c):
            earlier = earlier + jnp.where(owners[e] == owners[c], 1, 0)
        place.append(owners[c] * 2 + earlier)

    def dealt(rows, columns):
        second = lax.broadcasted_iota(jnp.int32, (rows, 128), 0) & 1
        slot = [place[c] - second for c in range(4)]

        def of(owner):
            total = jnp.zeros((rows, 128), jnp.float32)
            for c in range(4):
                total = jnp.where(slot[c] == 2 * owner, columns[c], total)
            return total

        return of

    def exchange(send, got, send_sem, recv_sem, d):
        return pltpu.make_async_remote_copy(
            src_ref=send.at[d],
            dst_ref=got.at[b],
            send_sem=send_sem,
            recv_sem=recv_sem,
            device_id=around(d),
            device_id_type=MESH,
        )

    def all_of(send, got, send_sem, recv_sem):
        return pltpu.make_async_remote_copy(
            src_ref=send.at[pl.ds(0, gy - 1)],
            dst_ref=got.at[pl.ds(0, gy - 1)],
            send_sem=send_sem,
            recv_sem=recv_sem,
            device_id=around(1),
            device_id_type=MESH,
        )

    u_exchange, v_exchange = (send_u, got_u, u_send, u_recv), (send_v, got_v, v_send, v_recv)
    far_first = sorted(range(1, gy), key=lambda d: -min(d, gy - d))

    of_u = dealt(8, [up[c] for c in range(4)])
    for d in far_first:
        send_u[d] = of_u(around(d)[1])
    got_u[b] = of_u(b)
    for dx, dy in SIDES:

        @pl.when(there(-dx, -dy))
        def _():
            for copy in copies[dx, dy]:
                copy.wait_recv()

    for dx in (-1, 0, 1):
        for dy in (-1, 0, 1):
            for axis in range(3):
                for i in range(2):
                    first = axis * 36 + (2 * dx + 2 + i) * 6 + 2 * dy + 2
                    rows = pos[place_of(dx, dy), axis, 2 * i : 2 * i + 2, :]
                    if (dx, dy) != (0, 0):
                        rows = jnp.where(there(dx, dy), rows, FAR)
                    grid_pos[first : first + 2, :] = rows

    rows16 = [
        (lax.broadcasted_iota(jnp.int32, (16, 128), 0) + 16 * k).astype(jnp.float32).astype(jnp.bfloat16)
        for k in range(8)
    ]
    one, none = jnp.ones((16, 128), jnp.bfloat16), jnp.zeros((16, 128), jnp.bfloat16)

    def column(k, part, total):
        x, y = 1 + k // 4, 1 + k % 4
        base = (x - 1) * 6 + y - 1
        entries = lists[k]
        slot, offset = entries & 127, entries >> 7
        near_by = [None] * 3
        for c in range(9):
            here = base + (c // 3) * 6 + c % 3
            for axis in range(3):
                source = jnp.broadcast_to(grid_pos[pl.ds(axis * 36 + here, 1), :], (8, 128))
                taken = jnp.take_along_axis(source, slot, axis=1)
                near_by[axis] = taken if c == 0 else jnp.where(offset == c, taken, near_by[axis])
        center = [
            jnp.broadcast_to(grid_pos[pl.ds(axis * 36 + base + 7, 1), :], (8, 128)) for axis in range(3)
        ]
        grads = column_terms(center, near_by)
        for axis in range(3):
            terms[k, axis] = grads[axis]
        highs = [g.astype(jnp.bfloat16).astype(jnp.float32) for g in grads]
        lows = [g - h for g, h in zip(grads, highs)]
        for t in range(4):
            cx, cy = 3 + t // 2 - x, 3 + t % 2 - y
            inside = (cx >= 0) & (cx <= 2) & (cy >= 0) & (cy <= 2)
            hit = offset == jnp.where(inside, 3 * cx + cy, -1)
            for axis in range(3):
                row = part * 192 + (t * 3 + axis) * 8
                split[pl.ds(row, 8), :] = jnp.where(hit, highs[axis], 0.0)
                split[pl.ds(row + 96, 8), :] = jnp.where(hit, lows[axis], 0.0)
        slot_f = slot.astype(jnp.float32)
        for m in range(0, 8, 2):
            left, right = [], []
            for e in (m, m + 1):
                left.append(split[pl.ds(part * 192 + e, 24, stride=8), :].astype(jnp.bfloat16))
                wanted = jnp.broadcast_to(slot_f[e : e + 1], (16, 128)).astype(jnp.bfloat16)
                right.append(
                    jnp.concatenate([jnp.where(r == wanted, one, none) for r in rows16], axis=0)
                )
            total = total + lax.dot_general(
                jnp.concatenate(left, axis=1),
                jnp.concatenate(right, axis=1),
                (((1,), (1,)), ((), ())),
                preferred_element_type=jnp.float32,
            )
        return total

    def some_columns(step, total):
        for part in range(UNROLL):
            total = column(step * UNROLL + part, part, total)
        return total

    for d in far_first:

        @pl.when((b + d >= (gy if d > 1 else 0)) & jnp.logical_not(waits_for_last))
        def _():
            exchange(*u_exchange, d).start()

    total = lax.fori_loop(0, 16 // UNROLL, some_columns, jnp.zeros((24, 128), jnp.float32))
    on_neighbours = total[0:12] + total[12:24]

    for t in range(4):
        own = 5 + 4 * (t // 2) + t % 2
        for axis in range(3):
            force = jnp.sum(terms[own, axis], axis=0, keepdims=True)
            force = force - on_neighbours[t * 3 + axis : t * 3 + axis + 1]
            speed = speed_v[t, axis : axis + 1, :] + half_step * (force * force_scale)
            vp[t, 2 * axis : 2 * axis + 2, :] = jnp.broadcast_to(speed, (2, 128))
    of_v = dealt(6, [vp[c] for c in range(4)])

    @pl.when(waits_for_last)
    def _():
        pl.semaphore_wait(known.at[2], 1)

    for d in far_first:
        send_v[d] = of_v(around(d)[1])

        @pl.when(b + d >= (gy if d > 1 else 0))
        def _():
            exchange(*v_exchange, d).start()

    got_v[b] = of_v(b)

    @pl.when(b <= half)
    def _():
        pl.semaphore_wait(known.at[2], 1)

    for d in range(1, gy):

        @pl.when((b + d >= (gy if d > 1 else 0)) & waits_for_last)
        def _():
            exchange(*u_exchange, d).start()

    for d in range(2, gy):

        @pl.when(b + d < gy)
        def _():
            exchange(*u_exchange, d).start()
            exchange(*v_exchange, d).start()

    all_of(*u_exchange).wait_recv()
    for o in range(gy):
        for r in range(4):
            out[0, 0, o, (0, 1, 2, 6)[r], :, :] = got_u[o, 2 * r : 2 * r + 2, :]
    for dx, dy in SIDES:

        @pl.when(there(dx, dy))
        def _():
            for copy in copies[dx, dy]:
                copy.wait_send()

    all_of(*u_exchange).wait_send()
    all_of(*v_exchange).wait_recv()
    for o in range(gy):
        for r in range(3):
            out[0, 0, o, r + 3, :, :] = got_v[o, 2 * r : 2 * r + 2, :]
    all_of(*v_exchange).wait_send()


def per_device(gx, gy, displacement, velocity, forces, heights, counts, neighbours, plan):
    dma = pltpu.SemaphoreType.DMA
    f32 = jnp.float32
    anywhere = pl.BlockSpec(memory_space=pltpu.HBM)
    inputs = [displacement, velocity, forces, heights, counts, neighbours, jnp.swapaxes(plan, 2, 3)]
    inputs = [pltpu.with_memory_space_constraint(value, pltpu.HBM) for value in inputs]
    arrived = pl.pallas_call(
        functools.partial(kernel, gx, gy),
        out_shape=jax.ShapeDtypeStruct((1, 1, gy, 7, 2, 128), f32),
        in_specs=[anywhere] * 7,
        out_specs=pl.BlockSpec(memory_space=pltpu.VMEM),
        scratch_shapes=[
            pltpu.VMEM((3, 2, 2, 128), f32),
            pltpu.VMEM((3, 2, 2, 128), f32),
            pltpu.VMEM((3, 2, 2, 128), f32),
            pltpu.VMEM((2, 2, 128), jnp.int32),
            pltpu.VMEM((8, 2, 2, 128), jnp.int32),
            pltpu.SMEM((2, 2), jnp.int32),
            pltpu.SMEM((1, 1, 1, 4), jnp.int32),
            pltpu.VMEM((9, 3, 4, 128), f32),
            pltpu.VMEM((112, 128), f32),
            pltpu.VMEM((16, 8, 128), jnp.int32),
            pltpu.VMEM((UNROLL * 192, 128), f32),
            pltpu.VMEM((16, 3, 8, 128), f32),
            pltpu.VMEM((4, 8, 128), f32),
            pltpu.VMEM((4, 8, 128), f32),
            pltpu.VMEM((4, 6, 128), f32),
            pltpu.VMEM((gy, 8, 128), f32),
            pltpu.VMEM((gy, 6, 128), f32),
            pltpu.VMEM((gy, 8, 128), f32),
            pltpu.VMEM((gy, 6, 128), f32),
            dma((7,)),
            dma((len(SIDES),)),
            dma((len(SIDES),)),
            dma((len(LISTS),)),
            dma((len(LISTS),)),
            dma,
            dma,
            dma,
            dma,
            pltpu.SemaphoreType.REGULAR((3,)),
        ],
        compiler_params=pltpu.CompilerParams(
            collective_id=0, has_side_effects=True, vmem_limit_bytes=VMEM_LIMIT
        ),
        name="verlet_recut",
    )(*inputs)
    return jnp.swapaxes(arrived, 3, 4)


def solution(mesh):
    in_specs = (
        P(None, "gx", "gy", None),
        P(None, "gx", "gy", None),
        P(None, "gx", "gy", None),
        P("gx", "gy", None),
        P("gx", "gy"),
        P(None, "gx", "gy", None),
        P("gx", "gy", None, None),
    )
    out_specs = P("gx", "gy", None, None, None, None)
    gx, gy = mesh.shape["gx"], mesh.shape["gy"]
    return jax.shard_map(
        functools.partial(per_device, gx, gy),
        mesh=mesh, in_specs=in_specs, out_specs=out_specs, check_vma=False,
    )
```

```python
import functools

import jax
import jax.numpy as jnp
from jax import lax
from jax.experimental import pallas as pl
from jax.experimental.pallas import tpu as pltpu
from jax.sharding import PartitionSpec as P

repulse_a = 1830.8
attract_b = 471.18
decay_one = 2.4799
decay_two = 1.7322
beta_t = 1.1e-06
expo_n = 0.78734
coeff_c2 = 100390.0**2
coeff_d2 = 16.217**2
coeff_h = -0.59825
spacing = 2.4
time_step = 0.001
half_step = 0.0005
force_scale = 9648.53 / 28.0855

FAR = 10000.0
MESH = pl.DeviceIdType.MESH
UNROLL = 4
VMEM_LIMIT = 8 * 1024 * 1024

SIDES = [(dx, dy) for dx in (-1, 0, 1) for dy in (-1, 0, 1) if (dx, dy) != (0, 0)]


CORNERS_FIRST = sorted(SIDES, key=lambda side: -abs(side[0]) - abs(side[1]))


def place_of(dx, dy):
    return (dx + 1) * 3 + dy + 1


def near(d):
    return {-1: (0,), 0: (0, 1), 1: (1,)}[d]


def poly_sin(x):
    y = x * x
    p = -1.0 / 39916800.0
    for c in (1.0 / 362880.0, -1.0 / 5040.0, 1.0 / 120.0, -1.0 / 6.0, 1.0):
        p = p * y + c
    return p * x


def poly_cos(x):
    y = x * x
    p = 1.0 / 479001600.0
    for c in (-1.0 / 3628800.0, 1.0 / 40320.0, -1.0 / 720.0, 1.0 / 24.0, -0.5, 1.0):
        p = p * y + c
    return p


def turn(x, by):
    return pltpu.roll(x, (8 - by) % 8, 0)


def above(value, limit):
    return jnp.where(value > limit, 1.0, jnp.where(value == limit, 0.5, 0.0))


def column_terms(center, near_by):
    occupied = jnp.where(center[2] < 0.5 * FAR, 0.5, 0.0)
    d = [q - p for q, p in zip(near_by, center)]
    square = d[0] * d[0] + d[1] * d[1] + d[2] * d[2]
    clipped = jnp.maximum(square, 1.0)
    inverse = lax.rsqrt(clipped)
    radius = clipped * inverse
    n = [c * inverse for c in d]
    angle = (jnp.clip(radius, 2.7, 3.0) - 2.85) * (0.5 * jnp.pi / 0.15)
    inner, outer = radius < 2.7, radius > 3.0
    w = jnp.where(inner, 1.0, jnp.where(outer, 0.0, 0.5 - 0.5 * poly_sin(angle)))
    slope = jnp.where(inner | outer, 0.0, poly_cos(angle) * (-0.25 * jnp.pi / 0.15))
    turned_n, turned_w, angular, dangular = {}, {}, {}, {}
    zeta = jnp.zeros_like(w)
    for by in (1, 2, 3, 4):
        tn = [turn(c, by) for c in n]
        tw = turn(w, by)
        cosine = n[0] * tn[0] + n[1] * tn[1] + n[2] * tn[2]
        apart = coeff_h - cosine
        spread = apart * apart
        part = 1.0 / (coeff_d2 + spread)
        g = 1.0 + (coeff_c2 / coeff_d2) * spread * part
        zeta = zeta + tw * g
        if by != 4:
            zeta = zeta + turn(w * g, 8 - by)
        turned_n[by], turned_w[by], angular[by] = tn, tw, g
        dangular[by] = (-2.0 * coeff_c2) * apart * (part * part)
    bond = jnp.maximum(zeta, 1.0)
    grown = jnp.exp(expo_n * jnp.log(beta_t * bond))
    order = jnp.exp((-0.5 / expo_n) * jnp.log(1.0 + grown))
    pull = attract_b * jnp.exp(-decay_two * radius)
    push = repulse_a * jnp.exp(-decay_one * radius)
    dzeta = (
        occupied * w * pull * (0.5 * order) * grown / ((1.0 + grown) * bond) * above(zeta, 1.0)
    )
    dw = occupied * (push - pull * order)
    dn = [jnp.zeros_like(w)] * 3
    for by in (1, 2, 3, 4):
        tz = turn(dzeta, by)
        pair = (dzeta * turned_w[by] + tz * w) * dangular[by]
        dw = dw + tz * angular[by]
        for axis in range(3):
            dn[axis] = dn[axis] + pair * turned_n[by][axis]
        if by != 4:
            dw = dw + turn(dzeta * angular[by], 8 - by)
            for axis in range(3):
                dn[axis] = dn[axis] + turn(pair * n[axis], 8 - by)
    dr = occupied * w * (decay_two * pull * order - decay_one * push) + dw * slope
    along = n[0] * dn[0] + n[1] * dn[1] + n[2] * dn[2]
    radial = (dr - along * inverse) * above(square, 1.0)
    return [dn[axis] * inverse + radial * n[axis] for axis in range(3)]


def kernel(
    gx, gy,
    displacement, velocity, forces, heights, counts, neighbours, plan,
    out,
    disp_v, vel_v, for_v, hei_v, nei_v, count_s, plan_s,
    pos, grid_pos, lists, split, terms, speed_v, up, vp, send_u, send_v, got_u, got_v,
    local_sem, pos_send, pos_recv, list_send, list_recv, u_send, u_recv, v_send, v_recv, known,
):
    a, b = lax.axis_index("gx"), lax.axis_index("gy")

    def at(da, db):
        return a + da, b + db

    def there(da, db):
        tests = {-1: a > 0, 0: None, 1: a < gx - 1}[da], {-1: b > 0, 0: None, 1: b < gy - 1}[db]
        tests = [t for t in tests if t is not None]
        return tests[0] if len(tests) == 1 else tests[0] & tests[1]

    barrier = pltpu.get_barrier_semaphore()
    def around(d):
        return a, lax.rem(b + d + gy, gy)

    for dx, dy in CORNERS_FIRST:
        if dx != 0:

            @pl.when(there(dx, dy))
            def _():
                pl.semaphore_signal(barrier, inc=1, device_id=at(dx, dy), device_id_type=MESH)

    pl.semaphore_signal(barrier, inc=1, device_id=around(-1), device_id_type=MESH)

    @pl.when(b < gy - 1)
    def _():
        pl.semaphore_signal(barrier, inc=1, device_id=around(1), device_id_type=MESH)

    loads = [
        pltpu.make_async_copy(source, target, local_sem.at[number])
        for number, (source, target) in enumerate(
            [
                (displacement, disp_v), (velocity, vel_v), (forces, for_v), (heights, hei_v),
                (neighbours, nei_v), (counts, count_s), (plan, plan_s),
            ]
        )
    ]
    for load in loads:
        load.start()
    for load in loads:
        load.wait()

    for i in range(2):
        high = hei_v[i]
        row = lax.broadcasted_iota(jnp.int32, (2, 128), 0)
        live = high < jnp.where(row == 0, count_s[i, 0], count_s[i, 1])
        occupied = live.astype(jnp.float32)
        for axis in range(3):
            speed = vel_v[axis, i] + half_step * (for_v[axis, i] * force_scale)
            offset = disp_v[axis, i] + time_step * speed
            if axis == 0:
                site = ((2 * a + i).astype(jnp.float32) + 0.5) * spacing
            elif axis == 1:
                site = ((2 * b + row).astype(jnp.float32) + 0.5) * spacing
            else:
                site = (high.astype(jnp.float32) + 0.5) * spacing
            where = site + offset
            if axis == 2:
                where = jnp.where(live, where, where + FAR)
            pos[4, axis, 2 * i : 2 * i + 2, :] = where
            for j in range(2):
                speed_v[2 * i + j, axis : axis + 1, :] = speed[j : j + 1]
                up[2 * i + j, 2 * axis : 2 * axis + 2, :] = jnp.broadcast_to(offset[j : j + 1], (2, 128))
        for j in range(2):
            up[2 * i + j, 6:8, :] = jnp.broadcast_to(occupied[j : j + 1], (2, 128))
            lists[1 + i, 1 + j] = nei_v[:, i, j, :]

    wide = (a > 0).astype(jnp.int32) + (a < gx - 1).astype(jnp.int32)
    high = 1 + (b > 0).astype(jnp.int32) + (b < gy - 1).astype(jnp.int32)
    pl.semaphore_wait(barrier, wide * high + 1 + (b > 0).astype(jnp.int32))

    copies = {side: [] for side in SIDES}
    for number, (dx, dy) in enumerate(SIDES):
        copies[dx, dy].append(
            pltpu.make_async_remote_copy(
                src_ref=pos.at[4],
                dst_ref=pos.at[place_of(-dx, -dy)],
                send_sem=pos_send.at[number],
                recv_sem=pos_recv.at[number],
                device_id=at(dx, dy),
                device_id_type=MESH,
            )
        )
    for number, (dx, dy) in enumerate(SIDES):
        here = tuple(pl.ds(1 + near(d)[0], len(near(d))) for d in (dx, dy))
        over = tuple(pl.ds(1 + near(d)[0] - 2 * d, len(near(d))) for d in (dx, dy))
        copies[dx, dy].append(
            pltpu.make_async_remote_copy(
                src_ref=lists.at[here],
                dst_ref=lists.at[over],
                send_sem=list_send.at[number],
                recv_sem=list_recv.at[number],
                device_id=at(dx, dy),
                device_id_type=MESH,
            )
        )
    for dx, dy in CORNERS_FIRST:

        @pl.when(there(dx, dy))
        def _():
            for copy in copies[dx, dy]:
                copy.start()

        @pl.when(jnp.logical_not(there(dx, dy)))
        def _():
            for i in near(-dx):
                for j in near(-dy):
                    lists[1 + i + 2 * dx, 1 + j + 2 * dy] = jnp.zeros((8, 128), jnp.int32)

    half = min(2 * gy // 3, gy - 2)

    def tell(number, target):
        pl.semaphore_signal(known.at[number], inc=1, device_id=(a, target), device_id_type=MESH)

    @pl.when(b >= 3)
    def _():
        pl.semaphore_wait(known.at[0], 1)

    @pl.when((b >= 2) & (b < gy - 1))
    def _():
        tell(0, b + 1)

    @pl.when(b == gy - 1)
    def _():
        for o in range(gy - 1):
            tell(2, o)

    @pl.when((b >= 2) & (b <= half))
    def _():
        pl.semaphore_wait(known.at[1], 1)

    @pl.when((b >= 1) & (b < half))
    def _():
        tell(1, b + 1)

    waits_for_last = (b > half) & (b < gy - 1)

    owners = [plan_s[0, 0, 0, c] for c in range(4)]
    place = []
    for c in range(4):
        earlier = jnp.int32(0)
        for e in range(c):
            earlier = earlier + jnp.where(owners[e] == owners[c], 1, 0)
        place.append(owners[c] * 2 + earlier)

    def dealt(rows, columns):
        second = lax.broadcasted_iota(jnp.int32, (rows, 128), 0) & 1
        slot = [place[c] - second for c in range(4)]

        def of(owner):
            total = jnp.zeros((rows, 128), jnp.float32)
            for c in range(4):
                total = jnp.where(slot[c] == 2 * owner, columns[c], total)
            return total

        return of

    def exchange(send, got, send_sem, recv_sem, d):
        return pltpu.make_async_remote_copy(
            src_ref=send.at[d],
            dst_ref=got.at[b],
            send_sem=send_sem,
            recv_sem=recv_sem,
            device_id=around(d),
            device_id_type=MESH,
        )

    def all_of(send, got, send_sem, recv_sem):
        return pltpu.make_async_remote_copy(
            src_ref=send.at[pl.ds(0, gy - 1)],
            dst_ref=got.at[pl.ds(0, gy - 1)],
            send_sem=send_sem,
            recv_sem=recv_sem,
            device_id=around(1),
            device_id_type=MESH,
        )

    u_exchange, v_exchange = (send_u, got_u, u_send, u_recv), (send_v, got_v, v_send, v_recv)
    far_first = sorted(range(1, gy), key=lambda d: -min(d, gy - d))

    of_u = dealt(8, [up[c] for c in range(4)])
    for d in far_first:
        send_u[d] = of_u(around(d)[1])
    got_u[b] = of_u(b)
    for dx, dy in SIDES:

        @pl.when(there(-dx, -dy))
        def _():
            for copy in copies[dx, dy]:
                copy.wait_recv()

    for dx in (-1, 0, 1):
        for dy in (-1, 0, 1):
            for axis in range(3):
                for i in range(2):
                    first = axis * 36 + (2 * dx + 2 + i) * 6 + 2 * dy + 2
                    rows = pos[place_of(dx, dy), axis, 2 * i : 2 * i + 2, :]
                    if (dx, dy) != (0, 0):
                        rows = jnp.where(there(dx, dy), rows, FAR)
                    grid_pos[first : first + 2, :] = rows

    rows16 = [
        (lax.broadcasted_iota(jnp.int32, (16, 128), 0) + 16 * k).astype(jnp.float32).astype(jnp.bfloat16)
        for k in range(8)
    ]
    one, none = jnp.ones((16, 128), jnp.bfloat16), jnp.zeros((16, 128), jnp.bfloat16)

    def gradients(k):
        x, y = 1 + k // 4, 1 + k % 4
        base = (x - 1) * 6 + y - 1
        entries = lists[k // 4, k % 4]
        slot, offset = entries & 127, entries >> 7
        near_by = [None] * 3
        for c in range(9):
            here = base + (c // 3) * 6 + c % 3
            for axis in range(3):
                source = jnp.broadcast_to(grid_pos[pl.ds(axis * 36 + here, 1), :], (8, 128))
                taken = jnp.take_along_axis(source, slot, axis=1)
                near_by[axis] = taken if c == 0 else jnp.where(offset == c, taken, near_by[axis])
        center = [
            jnp.broadcast_to(grid_pos[pl.ds(axis * 36 + base + 7, 1), :], (8, 128)) for axis in range(3)
        ]
        grads = column_terms(center, near_by)
        for axis in range(3):
            terms[k, axis] = grads[axis]

    def scattered(k, part, grads, total):
        x, y = 1 + k // 4, 1 + k % 4
        entries = lists[k // 4, k % 4]
        slot, offset = entries & 127, entries >> 7
        highs = [g.astype(jnp.bfloat16).astype(jnp.float32) for g in grads]
        lows = [g - h for g, h in zip(grads, highs)]
        for t in range(4):
            cx, cy = 3 + t // 2 - x, 3 + t % 2 - y
            inside = (cx >= 0) & (cx <= 2) & (cy >= 0) & (cy <= 2)
            hit = offset == jnp.where(inside, 3 * cx + cy, -1)
            for axis in range(3):
                row = part * 192 + (t * 3 + axis) * 8
                split[pl.ds(row, 8), :] = jnp.where(hit, highs[axis], 0.0)
                split[pl.ds(row + 96, 8), :] = jnp.where(hit, lows[axis], 0.0)
        slot_f = slot.astype(jnp.float32)
        for m in range(0, 8, 2):
            left, right = [], []
            for e in (m, m + 1):
                left.append(split[pl.ds(part * 192 + e, 24, stride=8), :].astype(jnp.bfloat16))
                wanted = jnp.broadcast_to(slot_f[e : e + 1], (16, 128)).astype(jnp.bfloat16)
                right.append(
                    jnp.concatenate([jnp.where(r == wanted, one, none) for r in rows16], axis=0)
                )
            total = total + lax.dot_general(
                jnp.concatenate(left, axis=1),
                jnp.concatenate(right, axis=1),
                (((1,), (1,)), ((), ())),
                preferred_element_type=jnp.float32,
            )
        return total

    def some_columns(step, total):
        before = [step * UNROLL - UNROLL + part for part in range(UNROLL)]
        grads = [[terms[k, axis] for axis in range(3)] for k in before]
        for part in range(UNROLL):
            total = scattered(before[part], part, grads[part], total)
            gradients(step * UNROLL + part)
        return total

    for d in far_first:

        @pl.when((b + d >= (gy if d > 1 else 0)) & jnp.logical_not(waits_for_last))
        def _():
            exchange(*u_exchange, d).start()

    for part in range(UNROLL):
        gradients(part)
    total = lax.fori_loop(1, 16 // UNROLL, some_columns, jnp.zeros((24, 128), jnp.float32))
    for part in range(UNROLL):
        k = 16 - UNROLL + part
        total = scattered(k, part, [terms[k, axis] for axis in range(3)], total)
    on_neighbours = total[0:12] + total[12:24]

    for t in range(4):
        own = 5 + 4 * (t // 2) + t % 2
        for axis in range(3):
            force = jnp.sum(terms[own, axis], axis=0, keepdims=True)
            force = force - on_neighbours[t * 3 + axis : t * 3 + axis + 1]
            speed = speed_v[t, axis : axis + 1, :] + half_step * (force * force_scale)
            vp[t, 2 * axis : 2 * axis + 2, :] = jnp.broadcast_to(speed, (2, 128))
    of_v = dealt(6, [vp[c] for c in range(4)])

    @pl.when(waits_for_last)
    def _():
        pl.semaphore_wait(known.at[2], 1)

    for d in far_first:
        send_v[d] = of_v(around(d)[1])

        @pl.when(b + d >= (gy if d > 1 else 0))
        def _():
            exchange(*v_exchange, d).start()

    got_v[b] = of_v(b)

    @pl.when(b <= half)
    def _():
        pl.semaphore_wait(known.at[2], 1)

    for d in range(1, gy):

        @pl.when((b + d >= (gy if d > 1 else 0)) & waits_for_last)
        def _():
            exchange(*u_exchange, d).start()

    for d in range(2, gy):

        @pl.when(b + d < gy)
        def _():
            exchange(*u_exchange, d).start()
            exchange(*v_exchange, d).start()

    all_of(*u_exchange).wait_recv()
    for o in range(gy):
        for r in range(4):
            out[0, 0, o, (0, 1, 2, 6)[r], :, :] = got_u[o, 2 * r : 2 * r + 2, :]
    for dx, dy in SIDES:

        @pl.when(there(dx, dy))
        def _():
            for copy in copies[dx, dy]:
                copy.wait_send()

    all_of(*u_exchange).wait_send()
    all_of(*v_exchange).wait_recv()
    for o in range(gy):
        for r in range(3):
            out[0, 0, o, r + 3, :, :] = got_v[o, 2 * r : 2 * r + 2, :]
    all_of(*v_exchange).wait_send()


def per_device(gx, gy, displacement, velocity, forces, heights, counts, neighbours, plan):
    dma = pltpu.SemaphoreType.DMA
    f32 = jnp.float32
    anywhere = pl.BlockSpec(memory_space=pltpu.HBM)
    inputs = [displacement, velocity, forces, heights, counts, neighbours, jnp.swapaxes(plan, 2, 3)]
    inputs = [pltpu.with_memory_space_constraint(value, pltpu.HBM) for value in inputs]
    arrived = pl.pallas_call(
        functools.partial(kernel, gx, gy),
        out_shape=jax.ShapeDtypeStruct((1, 1, gy, 7, 2, 128), f32),
        in_specs=[anywhere] * 7,
        out_specs=pl.BlockSpec(memory_space=pltpu.VMEM),
        scratch_shapes=[
            pltpu.VMEM((3, 2, 2, 128), f32),
            pltpu.VMEM((3, 2, 2, 128), f32),
            pltpu.VMEM((3, 2, 2, 128), f32),
            pltpu.VMEM((2, 2, 128), jnp.int32),
            pltpu.VMEM((8, 2, 2, 128), jnp.int32),
            pltpu.SMEM((2, 2), jnp.int32),
            pltpu.SMEM((1, 1, 1, 4), jnp.int32),
            pltpu.VMEM((9, 3, 4, 128), f32),
            pltpu.VMEM((112, 128), f32),
            pltpu.VMEM((4, 4, 8, 128), jnp.int32),
            pltpu.VMEM((UNROLL * 192, 128), f32),
            pltpu.VMEM((16, 3, 8, 128), f32),
            pltpu.VMEM((4, 8, 128), f32),
            pltpu.VMEM((4, 8, 128), f32),
            pltpu.VMEM((4, 6, 128), f32),
            pltpu.VMEM((gy, 8, 128), f32),
            pltpu.VMEM((gy, 6, 128), f32),
            pltpu.VMEM((gy, 8, 128), f32),
            pltpu.VMEM((gy, 6, 128), f32),
            dma((7,)),
            dma((len(SIDES),)),
            dma((len(SIDES),)),
            dma((len(SIDES),)),
            dma((len(SIDES),)),
            dma,
            dma,
            dma,
            dma,
            pltpu.SemaphoreType.REGULAR((3,)),
        ],
        compiler_params=pltpu.CompilerParams(
            collective_id=0, has_side_effects=True, vmem_limit_bytes=VMEM_LIMIT
        ),
        name="verlet_recut",
    )(*inputs)
    return jnp.swapaxes(arrived, 3, 4)


def solution(mesh):
    in_specs = (
        P(None, "gx", "gy", None),
        P(None, "gx", "gy", None),
        P(None, "gx", "gy", None),
        P("gx", "gy", None),
        P("gx", "gy"),
        P(None, "gx", "gy", None),
        P("gx", "gy", None, None),
    )
    out_specs = P("gx", "gy", None, None, None, None)
    gx, gy = mesh.shape["gx"], mesh.shape["gy"]
    return jax.shard_map(
        functools.partial(per_device, gx, gy),
        mesh=mesh, in_specs=in_specs, out_specs=out_specs, check_vma=False,
    )
```

```python
import functools

import jax
import jax.numpy as jnp
from jax import lax
from jax.experimental import pallas as pl
from jax.experimental.pallas import tpu as pltpu
from jax.sharding import PartitionSpec as P

repulse_a = 1830.8
attract_b = 471.18
decay_one = 2.4799
decay_two = 1.7322
beta_t = 1.1e-06
expo_n = 0.78734
coeff_c2 = 100390.0**2
coeff_d2 = 16.217**2
coeff_h = -0.59825
spacing = 2.4
time_step = 0.001
half_step = 0.0005
force_scale = 9648.53 / 28.0855

FAR = 10000.0
MESH = pl.DeviceIdType.MESH
UNROLL = 8
VMEM_LIMIT = 8 * 1024 * 1024

SIDES = [(dx, dy) for dx in (-1, 0, 1) for dy in (-1, 0, 1) if (dx, dy) != (0, 0)]


CORNERS_FIRST = sorted(SIDES, key=lambda side: -abs(side[0]) - abs(side[1]))


def place_of(dx, dy):
    return (dx + 1) * 3 + dy + 1


def near(d):
    return {-1: (0,), 0: (0, 1), 1: (1,)}[d]


def poly_sin(x):
    y = x * x
    p = -1.0 / 39916800.0
    for c in (1.0 / 362880.0, -1.0 / 5040.0, 1.0 / 120.0, -1.0 / 6.0, 1.0):
        p = p * y + c
    return p * x


def poly_cos(x):
    y = x * x
    p = 1.0 / 479001600.0
    for c in (-1.0 / 3628800.0, 1.0 / 40320.0, -1.0 / 720.0, 1.0 / 24.0, -0.5, 1.0):
        p = p * y + c
    return p


def turn(x, by):
    return pltpu.roll(x, (8 - by) % 8, 0)


def above(value, limit):
    return jnp.where(value > limit, 1.0, jnp.where(value == limit, 0.5, 0.0))


def column_terms(center, near_by):
    occupied = jnp.where(center[2] < 0.5 * FAR, 0.5, 0.0)
    d = [q - p for q, p in zip(near_by, center)]
    square = d[0] * d[0] + d[1] * d[1] + d[2] * d[2]
    clipped = jnp.maximum(square, 1.0)
    inverse = lax.rsqrt(clipped)
    radius = clipped * inverse
    n = [c * inverse for c in d]
    angle = (jnp.clip(radius, 2.7, 3.0) - 2.85) * (0.5 * jnp.pi / 0.15)
    inner, outer = radius < 2.7, radius > 3.0
    w = jnp.where(inner, 1.0, jnp.where(outer, 0.0, 0.5 - 0.5 * poly_sin(angle)))
    slope = jnp.where(inner | outer, 0.0, poly_cos(angle) * (-0.25 * jnp.pi / 0.15))
    turned_n, turned_w, angular, dangular = {}, {}, {}, {}
    zeta = jnp.zeros_like(w)
    for by in (1, 2, 3, 4):
        tn = [turn(c, by) for c in n]
        tw = turn(w, by)
        cosine = n[0] * tn[0] + n[1] * tn[1] + n[2] * tn[2]
        apart = coeff_h - cosine
        spread = apart * apart
        part = 1.0 / (coeff_d2 + spread)
        g = 1.0 + (coeff_c2 / coeff_d2) * spread * part
        zeta = zeta + tw * g
        if by != 4:
            zeta = zeta + turn(w * g, 8 - by)
        turned_n[by], turned_w[by], angular[by] = tn, tw, g
        dangular[by] = (-2.0 * coeff_c2) * apart * (part * part)
    bond = jnp.maximum(zeta, 1.0)
    grown = jnp.exp(expo_n * jnp.log(beta_t * bond))
    order = jnp.exp((-0.5 / expo_n) * jnp.log(1.0 + grown))
    pull = attract_b * jnp.exp(-decay_two * radius)
    push = repulse_a * jnp.exp(-decay_one * radius)
    dzeta = (
        occupied * w * pull * (0.5 * order) * grown / ((1.0 + grown) * bond) * above(zeta, 1.0)
    )
    dw = occupied * (push - pull * order)
    dn = [jnp.zeros_like(w)] * 3
    for by in (1, 2, 3, 4):
        tz = turn(dzeta, by)
        pair = (dzeta * turned_w[by] + tz * w) * dangular[by]
        dw = dw + tz * angular[by]
        for axis in range(3):
            dn[axis] = dn[axis] + pair * turned_n[by][axis]
        if by != 4:
            dw = dw + turn(dzeta * angular[by], 8 - by)
            for axis in range(3):
                dn[axis] = dn[axis] + turn(pair * n[axis], 8 - by)
    dr = occupied * w * (decay_two * pull * order - decay_one * push) + dw * slope
    along = n[0] * dn[0] + n[1] * dn[1] + n[2] * dn[2]
    radial = (dr - along * inverse) * above(square, 1.0)
    return [dn[axis] * inverse + radial * n[axis] for axis in range(3)]


def kernel(
    gx, gy,
    displacement, velocity, forces, heights, counts, neighbours, plan,
    out,
    disp_v, vel_v, for_v, hei_v, nei_v, count_s, plan_s,
    pos, grid_pos, lists, split, terms, speed_v, up, vp, send_u, send_v, got_u, got_v,
    local_sem, pos_send, pos_recv, list_send, list_recv, u_send, u_recv, v_send, v_recv, known,
):
    a, b = lax.axis_index("gx"), lax.axis_index("gy")

    def at(da, db):
        return a + da, b + db

    def there(da, db):
        tests = {-1: a > 0, 0: None, 1: a < gx - 1}[da], {-1: b > 0, 0: None, 1: b < gy - 1}[db]
        tests = [t for t in tests if t is not None]
        return tests[0] if len(tests) == 1 else tests[0] & tests[1]

    barrier = pltpu.get_barrier_semaphore()
    def around(d):
        return a, lax.rem(b + d + gy, gy)

    for dx, dy in CORNERS_FIRST:
        if dx != 0:

            @pl.when(there(dx, dy))
            def _():
                pl.semaphore_signal(barrier, inc=1, device_id=at(dx, dy), device_id_type=MESH)

    pl.semaphore_signal(barrier, inc=1, device_id=around(-1), device_id_type=MESH)

    @pl.when(b < gy - 1)
    def _():
        pl.semaphore_signal(barrier, inc=1, device_id=around(1), device_id_type=MESH)

    loads = [
        pltpu.make_async_copy(source, target, local_sem.at[number])
        for number, (source, target) in enumerate(
            [
                (displacement, disp_v), (velocity, vel_v), (forces, for_v), (heights, hei_v),
                (neighbours, nei_v), (counts, count_s), (plan, plan_s),
            ]
        )
    ]
    for load in loads:
        load.start()
    for load in loads:
        load.wait()

    for i in range(2):
        high = hei_v[i]
        row = lax.broadcasted_iota(jnp.int32, (2, 128), 0)
        live = high < jnp.where(row == 0, count_s[i, 0], count_s[i, 1])
        occupied = live.astype(jnp.float32)
        for axis in range(3):
            speed = vel_v[axis, i] + half_step * (for_v[axis, i] * force_scale)
            offset = disp_v[axis, i] + time_step * speed
            if axis == 0:
                site = ((2 * a + i).astype(jnp.float32) + 0.5) * spacing
            elif axis == 1:
                site = ((2 * b + row).astype(jnp.float32) + 0.5) * spacing
            else:
                site = (high.astype(jnp.float32) + 0.5) * spacing
            where = site + offset
            if axis == 2:
                where = jnp.where(live, where, where + FAR)
            pos[4, axis, 2 * i : 2 * i + 2, :] = where
            for j in range(2):
                speed_v[2 * i + j, axis : axis + 1, :] = speed[j : j + 1]
                up[2 * i + j, 2 * axis : 2 * axis + 2, :] = jnp.broadcast_to(offset[j : j + 1], (2, 128))
        for j in range(2):
            up[2 * i + j, 6:8, :] = jnp.broadcast_to(occupied[j : j + 1], (2, 128))
            lists[1 + i, 1 + j] = nei_v[:, i, j, :]

    wide = (a > 0).astype(jnp.int32) + (a < gx - 1).astype(jnp.int32)
    high = 1 + (b > 0).astype(jnp.int32) + (b < gy - 1).astype(jnp.int32)
    pl.semaphore_wait(barrier, wide * high + 1 + (b > 0).astype(jnp.int32))

    copies = {side: [] for side in SIDES}
    for number, (dx, dy) in enumerate(SIDES):
        copies[dx, dy].append(
            pltpu.make_async_remote_copy(
                src_ref=pos.at[4],
                dst_ref=pos.at[place_of(-dx, -dy)],
                send_sem=pos_send.at[number],
                recv_sem=pos_recv.at[number],
                device_id=at(dx, dy),
                device_id_type=MESH,
            )
        )
    for number, (dx, dy) in enumerate(SIDES):
        here = tuple(pl.ds(1 + near(d)[0], len(near(d))) for d in (dx, dy))
        over = tuple(pl.ds(1 + near(d)[0] - 2 * d, len(near(d))) for d in (dx, dy))
        copies[dx, dy].append(
            pltpu.make_async_remote_copy(
                src_ref=lists.at[here],
                dst_ref=lists.at[over],
                send_sem=list_send.at[number],
                recv_sem=list_recv.at[number],
                device_id=at(dx, dy),
                device_id_type=MESH,
            )
        )
    for dx, dy in CORNERS_FIRST:

        @pl.when(there(dx, dy))
        def _():
            for copy in copies[dx, dy]:
                copy.start()

        @pl.when(jnp.logical_not(there(dx, dy)))
        def _():
            for i in near(-dx):
                for j in near(-dy):
                    lists[1 + i + 2 * dx, 1 + j + 2 * dy] = jnp.zeros((8, 128), jnp.int32)

    half = min(2 * gy // 3, gy - 2)

    def tell(number, target):
        pl.semaphore_signal(known.at[number], inc=1, device_id=(a, target), device_id_type=MESH)

    @pl.when(b >= 3)
    def _():
        pl.semaphore_wait(known.at[0], 1)

    @pl.when((b >= 2) & (b < gy - 1))
    def _():
        tell(0, b + 1)

    @pl.when(b == gy - 1)
    def _():
        for o in range(gy - 1):
            tell(2, o)

    @pl.when((b >= 2) & (b <= half))
    def _():
        pl.semaphore_wait(known.at[1], 1)

    @pl.when((b >= 1) & (b < half))
    def _():
        tell(1, b + 1)

    waits_for_last = (b > half) & (b < gy - 1)

    owners = [plan_s[0, 0, 0, c] for c in range(4)]
    place = []
    for c in range(4):
        earlier = jnp.int32(0)
        for e in range(c):
            earlier = earlier + jnp.where(owners[e] == owners[c], 1, 0)
        place.append(owners[c] * 2 + earlier)

    def dealt(rows, columns):
        second = lax.broadcasted_iota(jnp.int32, (rows, 128), 0) & 1
        slot = [place[c] - second for c in range(4)]

        def of(owner):
            total = jnp.zeros((rows, 128), jnp.float32)
            for c in range(4):
                total = jnp.where(slot[c] == 2 * owner, columns[c], total)
            return total

        return of

    def exchange(send, got, send_sem, recv_sem, d):
        return pltpu.make_async_remote_copy(
            src_ref=send.at[d],
            dst_ref=got.at[b],
            send_sem=send_sem,
            recv_sem=recv_sem,
            device_id=around(d),
            device_id_type=MESH,
        )

    def all_of(send, got, send_sem, recv_sem):
        return pltpu.make_async_remote_copy(
            src_ref=send.at[pl.ds(0, gy - 1)],
            dst_ref=got.at[pl.ds(0, gy - 1)],
            send_sem=send_sem,
            recv_sem=recv_sem,
            device_id=around(1),
            device_id_type=MESH,
        )

    u_exchange, v_exchange = (send_u, got_u, u_send, u_recv), (send_v, got_v, v_send, v_recv)
    far_first = sorted(range(1, gy), key=lambda d: -min(d, gy - d))

    of_u = dealt(8, [up[c] for c in range(4)])
    for d in far_first:
        send_u[d] = of_u(around(d)[1])
    got_u[b] = of_u(b)
    for dx, dy in SIDES:

        @pl.when(there(-dx, -dy))
        def _():
            for copy in copies[dx, dy]:
                copy.wait_recv()

    for dx in (-1, 0, 1):
        for dy in (-1, 0, 1):
            for axis in range(3):
                for i in range(2):
                    first = axis * 36 + (2 * dx + 2 + i) * 6 + 2 * dy + 2
                    rows = pos[place_of(dx, dy), axis, 2 * i : 2 * i + 2, :]
                    if (dx, dy) != (0, 0):
                        rows = jnp.where(there(dx, dy), rows, FAR)
                    grid_pos[first : first + 2, :] = rows

    rows16 = [
        (lax.broadcasted_iota(jnp.int32, (16, 128), 0) + 16 * k).astype(jnp.float32).astype(jnp.bfloat16)
        for k in range(8)
    ]
    one, none = jnp.ones((16, 128), jnp.bfloat16), jnp.zeros((16, 128), jnp.bfloat16)

    def gradients(k):
        x, y = 1 + k // 4, 1 + k % 4
        base = (x - 1) * 6 + y - 1
        entries = lists[k // 4, k % 4]
        slot, offset = entries & 127, entries >> 7
        near_by = [None] * 3
        for c in range(9):
            here = base + (c // 3) * 6 + c % 3
            for axis in range(3):
                source = jnp.broadcast_to(grid_pos[pl.ds(axis * 36 + here, 1), :], (8, 128))
                taken = jnp.take_along_axis(source, slot, axis=1)
                near_by[axis] = taken if c == 0 else jnp.where(offset == c, taken, near_by[axis])
        center = [
            jnp.broadcast_to(grid_pos[pl.ds(axis * 36 + base + 7, 1), :], (8, 128)) for axis in range(3)
        ]
        grads = column_terms(center, near_by)
        for axis in range(3):
            terms[k, axis] = grads[axis]

    def scattered(k, part, grads, total):
        x, y = 1 + k // 4, 1 + k % 4
        entries = lists[k // 4, k % 4]
        slot, offset = entries & 127, entries >> 7
        highs = [g.astype(jnp.bfloat16).astype(jnp.float32) for g in grads]
        lows = [g - h for g, h in zip(grads, highs)]
        for t in range(4):
            cx, cy = 3 + t // 2 - x, 3 + t % 2 - y
            inside = (cx >= 0) & (cx <= 2) & (cy >= 0) & (cy <= 2)
            hit = offset == jnp.where(inside, 3 * cx + cy, -1)
            for axis in range(3):
                row = part * 192 + (t * 3 + axis) * 8
                split[pl.ds(row, 8), :] = jnp.where(hit, highs[axis], 0.0)
                split[pl.ds(row + 96, 8), :] = jnp.where(hit, lows[axis], 0.0)
        slot_f = slot.astype(jnp.float32)
        for m in range(0, 8, 2):
            left, right = [], []
            for e in (m, m + 1):
                left.append(split[pl.ds(part * 192 + e, 24, stride=8), :].astype(jnp.bfloat16))
                wanted = jnp.broadcast_to(slot_f[e : e + 1], (16, 128)).astype(jnp.bfloat16)
                right.append(
                    jnp.concatenate([jnp.where(r == wanted, one, none) for r in rows16], axis=0)
                )
            total = total + lax.dot_general(
                jnp.concatenate(left, axis=1),
                jnp.concatenate(right, axis=1),
                (((1,), (1,)), ((), ())),
                preferred_element_type=jnp.float32,
            )
        return total

    def some_columns(step, total):
        before = [step * UNROLL - UNROLL + part for part in range(UNROLL)]
        grads = [[terms[k, axis] for axis in range(3)] for k in before]
        for part in range(UNROLL):
            total = scattered(before[part], part, grads[part], total)
            gradients(step * UNROLL + part)
        return total

    for d in far_first:

        @pl.when((b + d >= (gy if d > 1 else 0)) & jnp.logical_not(waits_for_last))
        def _():
            exchange(*u_exchange, d).start()

    for part in range(UNROLL):
        gradients(part)
    total = some_columns(1, jnp.zeros((24, 128), jnp.float32))
    for part in range(UNROLL):
        k = 16 - UNROLL + part
        total = scattered(k, part, [terms[k, axis] for axis in range(3)], total)
    on_neighbours = total[0:12] + total[12:24]

    for t in range(4):
        own = 5 + 4 * (t // 2) + t % 2
        for axis in range(3):
            force = jnp.sum(terms[own, axis], axis=0, keepdims=True)
            force = force - on_neighbours[t * 3 + axis : t * 3 + axis + 1]
            speed = speed_v[t, axis : axis + 1, :] + half_step * (force * force_scale)
            vp[t, 2 * axis : 2 * axis + 2, :] = jnp.broadcast_to(speed, (2, 128))
    of_v = dealt(6, [vp[c] for c in range(4)])

    @pl.when(waits_for_last)
    def _():
        pl.semaphore_wait(known.at[2], 1)

    for d in far_first:
        send_v[d] = of_v(around(d)[1])

        @pl.when(b + d >= (gy if d > 1 else 0))
        def _():
            exchange(*v_exchange, d).start()

    got_v[b] = of_v(b)

    @pl.when(b <= half)
    def _():
        pl.semaphore_wait(known.at[2], 1)

    for d in range(1, gy):

        @pl.when((b + d >= (gy if d > 1 else 0)) & waits_for_last)
        def _():
            exchange(*u_exchange, d).start()

    for d in range(2, gy):

        @pl.when(b + d < gy)
        def _():
            exchange(*u_exchange, d).start()
            exchange(*v_exchange, d).start()

    all_of(*u_exchange).wait_recv()
    for o in range(gy):
        for r in range(4):
            out[0, 0, o, (0, 1, 2, 6)[r], :, :] = got_u[o, 2 * r : 2 * r + 2, :]
    for dx, dy in SIDES:

        @pl.when(there(dx, dy))
        def _():
            for copy in copies[dx, dy]:
                copy.wait_send()

    all_of(*u_exchange).wait_send()
    all_of(*v_exchange).wait_recv()
    for o in range(gy):
        for r in range(3):
            out[0, 0, o, r + 3, :, :] = got_v[o, 2 * r : 2 * r + 2, :]
    all_of(*v_exchange).wait_send()


def per_device(gx, gy, displacement, velocity, forces, heights, counts, neighbours, plan):
    dma = pltpu.SemaphoreType.DMA
    f32 = jnp.float32
    anywhere = pl.BlockSpec(memory_space=pltpu.HBM)
    inputs = [displacement, velocity, forces, heights, counts, neighbours, jnp.swapaxes(plan, 2, 3)]
    inputs = [pltpu.with_memory_space_constraint(value, pltpu.HBM) for value in inputs]
    arrived = pl.pallas_call(
        functools.partial(kernel, gx, gy),
        out_shape=jax.ShapeDtypeStruct((1, 1, gy, 7, 2, 128), f32),
        in_specs=[anywhere] * 7,
        out_specs=pl.BlockSpec(memory_space=pltpu.VMEM),
        scratch_shapes=[
            pltpu.VMEM((3, 2, 2, 128), f32),
            pltpu.VMEM((3, 2, 2, 128), f32),
            pltpu.VMEM((3, 2, 2, 128), f32),
            pltpu.VMEM((2, 2, 128), jnp.int32),
            pltpu.VMEM((8, 2, 2, 128), jnp.int32),
            pltpu.SMEM((2, 2), jnp.int32),
            pltpu.SMEM((1, 1, 1, 4), jnp.int32),
            pltpu.VMEM((9, 3, 4, 128), f32),
            pltpu.VMEM((112, 128), f32),
            pltpu.VMEM((4, 4, 8, 128), jnp.int32),
            pltpu.VMEM((UNROLL * 192, 128), f32),
            pltpu.VMEM((16, 3, 8, 128), f32),
            pltpu.VMEM((4, 8, 128), f32),
            pltpu.VMEM((4, 8, 128), f32),
            pltpu.VMEM((4, 6, 128), f32),
            pltpu.VMEM((gy, 8, 128), f32),
            pltpu.VMEM((gy, 6, 128), f32),
            pltpu.VMEM((gy, 8, 128), f32),
            pltpu.VMEM((gy, 6, 128), f32),
            dma((7,)),
            dma((len(SIDES),)),
            dma((len(SIDES),)),
            dma((len(SIDES),)),
            dma((len(SIDES),)),
            dma,
            dma,
            dma,
            dma,
            pltpu.SemaphoreType.REGULAR((3,)),
        ],
        compiler_params=pltpu.CompilerParams(
            collective_id=0, has_side_effects=True, vmem_limit_bytes=VMEM_LIMIT
        ),
        name="verlet_recut",
    )(*inputs)
    return jnp.swapaxes(arrived, 3, 4)


def solution(mesh):
    in_specs = (
        P(None, "gx", "gy", None),
        P(None, "gx", "gy", None),
        P(None, "gx", "gy", None),
        P("gx", "gy", None),
        P("gx", "gy"),
        P(None, "gx", "gy", None),
        P("gx", "gy", None, None),
    )
    out_specs = P("gx", "gy", None, None, None, None)
    gx, gy = mesh.shape["gx"], mesh.shape["gy"]
    return jax.shard_map(
        functools.partial(per_device, gx, gy),
        mesh=mesh, in_specs=in_specs, out_specs=out_specs, check_vma=False,
    )
```
